32 devices in a mesh: seq: 4 (over z), fsdp: 8 (over y, x, core).
Axes of the slice: x: 2, y: 2, z: 4, core: 2. Of those that a mesh axis runs over, the one named last changes fastest.
Arguments:
- tokens: bfloat16 [8, 1024, 1152], P('fsdp', 'seq'), may hold values from -6 to 6
- pre_attn_gain: float32 [1152], replicated, may hold values from 0.1 to 1.9
- qkv_weight: bfloat16 [1152, 4096], P('fsdp'), may hold values from -0.1875 to 0.1875
- out_weight: bfloat16 [2048, 1152], P('fsdp'), may hold values from -0.125 to 0.125
- post_attn_gain: float32 [1152], replicated, may hold values from 0.1 to 1.9
- pre_ffn_gain: float32 [1152], replicated, may hold values from 0.1 to 1.9
- gate_up_weight: bfloat16 [1152, 13824], P('fsdp'), may hold values from -0.1875 to 0.1875
- down_weight: bfloat16 [6912, 1152], P('fsdp'), may hold values from -0.078125 to 0.078125
- post_ffn_gain: float32 [1152], replicated, may hold values from 0.1 to 1.9
- out_grad: bfloat16 [8, 1024, 1152], P('fsdp', 'seq'), may hold values from -6 to 6
Outputs:
- layer_out: bfloat16 [8, 1024, 1152], P('fsdp', 'seq')
- tokens_grad: float32 [8, 1024, 1152], P('fsdp', 'seq')
- pre_attn_gain_grad: float32 [1152], replicated
- qkv_weight_grad: float32 [1152, 4096], P('fsdp')
- out_weight_grad: float32 [2048, 1152], P('fsdp')
- post_attn_gain_grad: float32 [1152], replicated
- pre_ffn_gain_grad: float32 [1152], replicated
- gate_up_weight_grad: float32 [1152, 13824], P('fsdp')
- down_weight_grad: float32 [6912, 1152], P('fsdp')
- post_ffn_gain_grad: float32 [1152], replicated
The draws below stay inside these ranges and needn't reach their ends.
All inputs are finite; a program needn't handle non-finite values.
Results may differ from the reference program's by a relative error of at most 0.02.
Values may be sent and summed in bfloat16 or wider, within the bound.
A program may use at most 320 MiB of HBM per device.

```python
import math
import jax
import jax.numpy as jnp
from jax import lax

D = 1152
H = 8
KV = 4
HD = 256
FF = 6912
LEN = 1024
SEQS = 8
QKV = 4096


def block_levels(key, extent, pieces, low, largest):
    gain, own = 1.0, jax.random.fold_in(key, 6)
    for dim, blocks in pieces:
        draws = jnp.exp(jax.random.uniform(jax.random.fold_in(own, dim), (blocks,), jnp.float32, low / len(pieces), largest / len(pieces)))
        gain = gain * jnp.repeat(draws, extent[dim] // blocks).reshape([-1 if axis == dim else 1 for axis in range(len(extent))])
    return gain


def bell_draw(stream_key, dims, scale, reach, pieces=(), kind=jnp.bfloat16):
    entries = scale * jax.random.normal(stream_key, dims, jnp.float32)
    if pieces:
        entries = entries * block_levels(stream_key, dims, pieces, -0.22, 0.18)
    return jnp.clip(entries, -reach, reach).astype(kind)


def setup_inputs(seed: int = 0) -> dict:
    seeds = jax.random.split(jax.random.key(seed), 11)
    tokens = bell_draw(seeds[0], (SEQS, LEN, D), 1.0, 6.0, ((0, 8), (1, 4)))
    pre_attn_gain = jnp.clip(1.0 + 0.18 * jax.random.normal(seeds[1], (D,), jnp.float32), 0.1, 1.9)
    qkv_weight = bell_draw(seeds[2], (D, QKV), D ** -0.5, 0.1875, ((0, 8),))
    out_weight = bell_draw(seeds[3], (H * HD, D), (H * HD) ** -0.5, 0.125, ((0, 8),))
    post_attn_gain = jnp.clip(1.0 + 0.18 * jax.random.normal(seeds[4], (D,), jnp.float32), 0.1, 1.9)
    pre_ffn_gain = jnp.clip(1.0 + 0.18 * jax.random.normal(seeds[5], (D,), jnp.float32), 0.1, 1.9)
    gate_up_weight = bell_draw(seeds[6], (D, 2 * FF), D ** -0.5, 0.1875, ((0, 8),))
    down_weight = bell_draw(seeds[7], (FF, D), FF ** -0.5, 0.078125, ((0, 8),))
    post_ffn_gain = jnp.clip(1.0 + 0.18 * jax.random.normal(seeds[8], (D,), jnp.float32), 0.1, 1.9)
    out_grad = bell_draw(seeds[9], (SEQS, LEN, D), 1.0, 6.0, ((0, 8), (1, 4)))
    return dict(tokens=tokens, pre_attn_gain=pre_attn_gain, qkv_weight=qkv_weight, out_weight=out_weight, post_attn_gain=post_attn_gain, pre_ffn_gain=pre_ffn_gain, gate_up_weight=gate_up_weight, down_weight=down_weight, post_ffn_gain=post_ffn_gain, out_grad=out_grad)


EPSILON = 1e-06
SOFT_CAP = 50.0
QUERY_FACTOR = 0.0625
GELU_COEFF = math.sqrt(2.0 / math.pi)
CUBIC = 0.044715
MASKED = -1e+30

def inverse_rms(values):
    return lax.rsqrt(lax.optimization_barrier(jnp.mean(values * values, axis=-1, keepdims=True)) + EPSILON)

def norm_back(upstream, values, inv_scale, gains):
    weighted = upstream * gains
    inner_mean = lax.optimization_barrier(jnp.mean(weighted * values, axis=-1, keepdims=True))
    gradient = inv_scale * weighted - values * (inv_scale * inv_scale * inv_scale) * inner_mean
    gain_grad = lax.optimization_barrier(jnp.sum(upstream * values * inv_scale, axis=0))
    return (gradient, gain_grad)

def gelu_pair(values):
    inner_part = GELU_COEFF * (values + CUBIC * values * values * values)
    tanh_part = jnp.tanh(inner_part)
    activated = 0.5 * values * (1.0 + tanh_part)
    derivative = 0.5 * (1.0 + tanh_part) + 0.5 * values * (1.0 - tanh_part * tanh_part) * GELU_COEFF * (1.0 + 3.0 * CUBIC * values * values)
    return (activated, derivative)

def batched_contraction(pattern, left_side, right_side):
    return jnp.einsum(pattern, left_side.astype(jnp.float32), right_side.astype(jnp.float32))

def matmul(left_side, right_side):
    return jnp.dot(left_side, right_side, preferred_element_type=jnp.float32)

def capped_scores(block_of_queries, key_row_slices, offset):
    amount = block_of_queries.shape[0]
    key_count = key_row_slices.shape[0]
    unscaled_logits = batched_contraction('olv,ilv->loi', block_of_queries, key_row_slices) * QUERY_FACTOR
    tanh_part = jnp.tanh(unscaled_logits / SOFT_CAP)
    allowed = jnp.arange(key_count, dtype=jnp.int32)[None, :] <= (offset + jnp.arange(amount, dtype=jnp.int32))[:, None]
    capped = jnp.where(allowed[None], SOFT_CAP * tanh_part, MASKED)
    return (tanh_part, capped)

def attend(queries, key_row_slices, value_row_slices):
    length = queries.shape[0]
    block_size = min(512, length)
    blocks = length // block_size

    def one_block(block_id):
        offset = block_id * block_size
        block_of_queries = lax.dynamic_slice_in_dim(queries, offset, block_size, 0)
        tanh_part, capped = capped_scores(block_of_queries, key_row_slices, offset)
        biggest = lax.optimization_barrier(jnp.max(capped, axis=-1, keepdims=True))
        logsum = biggest + jnp.log(lax.optimization_barrier(jnp.sum(jnp.exp(capped - biggest), axis=-1, keepdims=True)))
        attention_probabilities = jnp.exp(capped - logsum).astype(jnp.bfloat16)
        layer_result = batched_contraction('vxn,nvs->xvs', attention_probabilities, value_row_slices).astype(jnp.bfloat16)
        return (layer_result, logsum[..., 0])
    outputs, logsums = lax.map(one_block, jnp.arange(blocks, dtype=jnp.int32))
    return (outputs.reshape(queries.shape), logsums)

def attend_back(queries, key_row_slices, value_row_slices, outputs, out_delta, logsums):
    length = queries.shape[0]
    block_size = min(512, length)
    blocks = length // block_size
    row_dots = batched_contraction('qbd,qbd->bq', out_delta, outputs)

    def one_block(carried, inputs):
        key_accumulator, value_accumulator = carried
        block_id, block_logsum = inputs
        offset = block_id * block_size
        block_of_queries = lax.dynamic_slice_in_dim(queries, offset, block_size, 0)
        block_correction = lax.dynamic_slice_in_dim(out_delta, offset, block_size, 0)
        tanh_part, capped = capped_scores(block_of_queries, key_row_slices, offset)
        attention_probabilities = jnp.exp(capped - block_logsum[..., None])
        probability_gradients = batched_contraction('olv,ilv->loi', block_correction, value_row_slices)
        dots_block = lax.dynamic_slice_in_dim(row_dots, offset, block_size, 1)
        logit_gradients = (attention_probabilities * (probability_gradients - dots_block[..., None]) * (1.0 - tanh_part * tanh_part) * QUERY_FACTOR).astype(jnp.bfloat16)
        rounded_values = attention_probabilities.astype(jnp.bfloat16)
        value_accumulator = value_accumulator + batched_contraction('pfm,fpg->mpg', rounded_values, block_correction)
        key_accumulator = key_accumulator + batched_contraction('pfm,fpg->mpg', logit_gradients, block_of_queries)
        query_gradient = batched_contraction('vxn,nvs->xvs', logit_gradients, key_row_slices).astype(jnp.bfloat16)
        return ((key_accumulator, value_accumulator), query_gradient)
    zero_acc = jnp.zeros(key_row_slices.shape, jnp.float32)
    (key_accumulator, value_accumulator), query_grads = lax.scan(one_block, (zero_acc, zero_acc), (jnp.arange(blocks, dtype=jnp.int32), logsums))
    return (query_grads.reshape(queries.shape), key_accumulator.astype(jnp.bfloat16), value_accumulator.astype(jnp.bfloat16))

def layer_sequence(seq_tokens, seq_grad, pre_attn_gain, qkv_weight, out_weight, post_attn_gain, pre_ffn_gain, gate_up_weight, down_weight, post_ffn_gain):
    length = seq_tokens.shape[0]
    head_repeat = H // KV
    residual_in = seq_tokens.astype(jnp.float32)
    scale_one = inverse_rms(residual_in)
    normed_in = (residual_in * scale_one * pre_attn_gain).astype(jnp.bfloat16)
    projected = matmul(normed_in, qkv_weight).astype(jnp.bfloat16)
    queries = projected[:, :H * HD].reshape(length, H, HD)
    key_row_slices = jnp.repeat(projected[:, H * HD:(H + KV) * HD].reshape(length, KV, HD), head_repeat, axis=1)
    value_row_slices = jnp.repeat(projected[:, (H + KV) * HD:].reshape(length, KV, HD), head_repeat, axis=1)
    head_out, logsums = attend(queries, key_row_slices, value_row_slices)
    attn_out = head_out.reshape(length, H * HD)
    branch_one = matmul(attn_out, out_weight)
    scale_two = inverse_rms(branch_one)
    hidden = residual_in + branch_one * scale_two * post_attn_gain
    scale_three = inverse_rms(hidden)
    normed_mid = (hidden * scale_three * pre_ffn_gain).astype(jnp.bfloat16)
    gate_up = matmul(normed_mid, gate_up_weight)
    gate_part = gate_up[:, :FF]
    up_part = gate_up[:, FF:]
    activated, derivative = gelu_pair(gate_part)
    mixed = (activated * up_part).astype(jnp.bfloat16)
    branch_two = matmul(mixed, down_weight)
    scale_four = inverse_rms(branch_two)
    layer_out = (hidden + branch_two * scale_four * post_ffn_gain).astype(jnp.bfloat16)
    upstream = seq_grad.astype(jnp.float32)
    branch_two_grad, post_ffn_term = norm_back(upstream, branch_two, scale_four, post_ffn_gain)
    branch_two_grad = branch_two_grad.astype(jnp.bfloat16)
    down_grad = matmul(mixed.T, branch_two_grad)
    mixed_grad = matmul(branch_two_grad, down_weight.T)
    gate_up_grad = jnp.concatenate([mixed_grad * up_part * derivative, mixed_grad * activated], axis=1).astype(jnp.bfloat16)
    gate_up_wgrad = matmul(normed_mid.T, gate_up_grad)
    normed_mid_grad = matmul(gate_up_grad, gate_up_weight.T)
    hidden_part, pre_ffn_term = norm_back(normed_mid_grad, hidden, scale_three, pre_ffn_gain)
    hidden_grad = upstream + hidden_part
    branch_one_grad, post_attn_term = norm_back(hidden_grad, branch_one, scale_two, post_attn_gain)
    branch_one_grad = branch_one_grad.astype(jnp.bfloat16)
    out_wgrad = matmul(attn_out.T, branch_one_grad)
    attn_grad = matmul(branch_one_grad, out_weight.T).astype(jnp.bfloat16).reshape(length, H, HD)
    query_gradient, key_grad, value_grad = attend_back(queries, key_row_slices, value_row_slices, head_out, attn_grad, logsums)
    key_sum = key_grad.astype(jnp.float32).reshape(length, KV, head_repeat, HD).sum(axis=2).astype(jnp.bfloat16)
    value_sum = value_grad.astype(jnp.float32).reshape(length, KV, head_repeat, HD).sum(axis=2).astype(jnp.bfloat16)
    qkv_grad = jnp.concatenate([query_gradient.reshape(length, H * HD), key_sum.reshape(length, KV * HD), value_sum.reshape(length, KV * HD)], axis=1)
    qkv_wgrad = matmul(normed_in.T, qkv_grad)
    normed_in_grad = matmul(qkv_grad, qkv_weight.T)
    input_part, pre_attn_term = norm_back(normed_in_grad, residual_in, scale_one, pre_attn_gain)
    tokens_grad = hidden_grad + input_part
    return (layer_out, tokens_grad, (qkv_wgrad, out_wgrad, gate_up_wgrad, down_grad), (pre_attn_term, post_attn_term, pre_ffn_term, post_ffn_term))

def reference(tokens, pre_attn_gain, qkv_weight, out_weight, post_attn_gain, pre_ffn_gain, gate_up_weight, down_weight, post_ffn_gain, out_grad):

    def step(carried, inputs):
        seq_tokens, seq_grad = inputs
        layer_out, tokens_grad, weight_terms, gain_terms = layer_sequence(seq_tokens, seq_grad, pre_attn_gain, qkv_weight, out_weight, post_attn_gain, pre_ffn_gain, gate_up_weight, down_weight, post_ffn_gain)
        carried = jax.tree.map(lambda running, extra: running + extra, carried, (weight_terms, gain_terms))
        return (carried, (layer_out, tokens_grad))
    weight_zeros = (jnp.zeros((D, QKV), jnp.float32), jnp.zeros((H * HD, D), jnp.float32), jnp.zeros((D, 2 * FF), jnp.float32), jnp.zeros((FF, D), jnp.float32))
    gain_zeros = (jnp.zeros((D,), jnp.float32), jnp.zeros((D,), jnp.float32), jnp.zeros((D,), jnp.float32), jnp.zeros((D,), jnp.float32))
    (weight_sums, gain_sums), (layer_out, tokens_grad) = lax.scan(step, (weight_zeros, gain_zeros), (tokens, out_grad))
    return (layer_out, tokens_grad, gain_sums[0], weight_sums[0], weight_sums[1], gain_sums[1], gain_sums[2], weight_sums[2], weight_sums[3], gain_sums[3])
```

```python
import functools
import math

import jax
import jax.numpy as jnp
from jax import lax
from jax.experimental import pallas as pl
from jax.experimental.pallas import tpu as pltpu
from jax.sharding import PartitionSpec as P

H = 8
KV = 4
HD = 256

EPSILON = 1e-06
SOFT_CAP = 50.0
QUERY_FACTOR = 0.0625
GELU_COEFF = math.sqrt(2.0 / math.pi)
CUBIC = 0.044715
MASKED = -1e30
MESH = pl.DeviceIdType.MESH
F32 = jnp.float32
BF16 = jnp.bfloat16
LANES = 128


def inverse_rms(values):
    return lax.rsqrt(jnp.mean(values * values, axis=-1, keepdims=True) + EPSILON)


def norm_back(upstream, values, inv_scale, gains):
    weighted = upstream * gains
    inner_mean = jnp.mean(weighted * values, axis=-1, keepdims=True)
    gradient = inv_scale * weighted - values * (inv_scale * inv_scale * inv_scale) * inner_mean
    gain_grad = jnp.sum(upstream * values * inv_scale, axis=0, keepdims=True)
    return (gradient, gain_grad)


def gelu_pair(values):
    inner_part = GELU_COEFF * (values + CUBIC * values * values * values)
    tanh_part = jnp.tanh(inner_part)
    activated = 0.5 * values * (1.0 + tanh_part)
    derivative = 0.5 * (1.0 + tanh_part) + 0.5 * values * (
        1.0 - tanh_part * tanh_part
    ) * GELU_COEFF * (1.0 + 3.0 * CUBIC * values * values)
    return (activated, derivative)


def plane_kernel(reduce, gather, n_in, n_own, body, *refs):
    refs = list(refs)
    part = refs.pop(0) if reduce else None
    ins = [refs.pop(0) for _ in range(n_in)]
    full = refs.pop(0) if gather else None
    outs = [refs.pop(0) for _ in range(n_own)]
    if reduce:
        acc, other, ra, rb, rx, ry = (refs.pop(0) for _ in range(6))
    block = refs.pop(0) if gather else None
    lsem, ssem, rsem = refs
    rows = ins[0].shape[0]
    half = rows // 2
    halves = (pl.ds(0, half), pl.ds(half, half))

    me = lax.axis_index("fsdp")
    core, xpos, ypos = me % 2, (me // 2) % 2, me // 4
    step = 1 - 2 * core
    mate = me + step
    xn = me + 2 - 4 * xpos
    yn = me + 4 - 8 * ypos
    diag = xn + 4 - 8 * ypos

    counter = [0]
    waits = []

    def send(src, dst, to):
        k = counter[0]
        counter[0] += 1
        copy = pltpu.make_async_remote_copy(
            src_ref=src, dst_ref=dst, send_sem=ssem.at[k], recv_sem=rsem.at[k],
            device_id={"fsdp": to}, device_id_type=MESH,
        )
        copy.start()
        waits.append(copy)
        return copy

    locals_ = []

    def local(src, dst):
        copy = pltpu.make_async_copy(src, dst, lsem.at[len(locals_)])
        copy.start()
        locals_.append(copy)
        return copy

    if reduce:
        order = (diag, xn, yn, me)
        own = [local(part.at[:, b], acc.at[k]) for k, b in enumerate(order)]

    barrier = pltpu.get_barrier_semaphore()
    for to in (mate, xn, yn):
        pl.semaphore_signal(barrier, inc=1, device_id={"fsdp": to}, device_id_type=MESH)
    pl.semaphore_wait(barrier, 3)

    if reduce:
        mates = [send(part.at[:, b + step], other.at[k], mate) for k, b in enumerate(order)]

        def add(dst, src, lo, count):
            def one(i, _):
                dst[lo + i] = (dst[lo + i].astype(F32) + src[i].astype(F32)).astype(BF16)
                return 0

            lax.fori_loop(0, count, one, 0)

        def join(k):
            own[k].wait()
            mates[k].wait_recv()
            add(acc.at[k], other.at[k], 0, rows)

        join(0)
        ca = send(acc.at[0, halves[0]], ra, yn)
        cb = send(acc.at[0, halves[1]], rb, xn)
        join(1)
        cx1 = send(acc.at[1, halves[1]], rx.at[halves[1]], xn)
        join(2)
        cy0 = send(acc.at[2, halves[0]], ry.at[halves[0]], yn)
        ca.wait_recv()
        add(acc.at[1], ra, 0, half)
        cx0 = send(acc.at[1, halves[0]], rx.at[halves[0]], xn)
        cb.wait_recv()
        add(acc.at[2], rb, half, half)
        cy1 = send(acc.at[2, halves[1]], ry.at[halves[1]], yn)
        own[3].wait()
        mates[3].wait_recv()
        for copy in (cx1, cy0, cx0, cy1):
            copy.wait_recv()

    def one(i, sums):
        if reduce:
            total = (
                acc[3, i].astype(F32) + other[3, i].astype(F32)
            ) + (rx[i].astype(F32) + ry[i].astype(F32))
        else:
            total = None
        sent, extra = body(i, total, ins, outs)
        if gather:
            block[i] = sent
        if extra is None:
            return sums
        return tuple(s + e for s, e in zip(sums, extra))

    width = ins[0].shape[-1]
    n_sums = body.n_sums
    sums = lax.fori_loop(0, rows, one, tuple(jnp.zeros((1, width), F32) for _ in range(n_sums)))
    for s, ref in zip(sums, outs[n_own - n_sums :]):
        ref[...] = s

    if gather:
        keep = local(block, full.at[:, me])
        h0, h1 = halves

        def forward(copy, where, blk, to):
            copy.wait_recv()
            return send(full.at[where, blk], full.at[where, blk], to)

        y0 = send(block.at[h0], full.at[h0, me], yn)
        x1 = send(block.at[h1], full.at[h1, me], xn)
        y1 = send(block.at[h1], full.at[h1, me], yn)
        x0 = send(block.at[h0], full.at[h0, me], xn)
        m = send(block, full.at[:, me], mate)
        gx = forward(y0, h0, yn, xn)
        fy0 = send(full.at[h0, yn], full.at[h0, yn], mate)
        gy = forward(x1, h1, xn, yn)
        fx1 = send(full.at[h1, xn], full.at[h1, xn], mate)
        forward(y1, h1, yn, mate)
        forward(x0, h0, xn, mate)
        forward(gx, h0, diag, mate)
        forward(gy, h1, diag, mate)
        for copy in (m, fy0, fx1):
            copy.wait_recv()
        for copy in waits[-4:]:
            copy.wait_recv()
        keep.wait()
    for copy in waits:
        copy.wait_send()


def plane_call(name, cid, body, part, ins, own_types, gather, planes, width):
    reduce = part is not None
    rows, r = ins[0].shape[0], ins[0].shape[1]
    shape = (rows, r, width)
    out_shape, out_specs = [], []
    if gather:
        out_shape.append(jax.ShapeDtypeStruct((rows, planes, r, width), BF16))
        out_specs.append(pl.BlockSpec(memory_space=pl.ANY))
    for t in own_types:
        out_shape.append(jax.ShapeDtypeStruct(shape, t))
        out_specs.append(pl.BlockSpec(memory_space=pltpu.VMEM))
    for _ in range(body.n_sums):
        out_shape.append(jax.ShapeDtypeStruct((1, width), F32))
        out_specs.append(pl.BlockSpec(memory_space=pltpu.VMEM))
    scratch = []
    if reduce:
        hs = (rows // 2, r, width)
        scratch += [pltpu.VMEM((4,) + shape, BF16)] * 2 + [pltpu.VMEM(hs, BF16)] * 2
        scratch += [pltpu.VMEM(shape, BF16)] * 2
    if gather:
        scratch.append(pltpu.VMEM(shape, BF16))
    n_send = (10 if reduce else 0) + (13 if gather else 0)
    scratch += [
        pltpu.SemaphoreType.DMA((5,)),
        pltpu.SemaphoreType.DMA((n_send,)),
        pltpu.SemaphoreType.DMA((n_send,)),
    ]
    operands = ([part] if reduce else []) + list(ins)
    in_specs = ([pl.BlockSpec(memory_space=pl.ANY)] if reduce else []) + [
        pl.BlockSpec(memory_space=pltpu.VMEM)
    ] * len(ins)
    return pl.pallas_call(
        functools.partial(
            plane_kernel, reduce, gather, len(ins), len(own_types) + body.n_sums, body
        ),
        name=name,
        out_shape=out_shape,
        in_specs=in_specs,
        out_specs=out_specs,
        scratch_shapes=scratch,
        compiler_params=pltpu.CompilerParams(collective_id=cid, has_side_effects=True),
    )(*operands)


def with_sums(n):
    def mark(f):
        f.n_sums = n
        return f

    return mark


@with_sums(0)
def body_first(i, _, ins, outs):
    tokens, gain = ins
    values = tokens[i].astype(F32)
    return (values * inverse_rms(values) * gain[...]).astype(BF16), None


@with_sums(0)
def body_mid(i, branch, ins, outs):
    tokens, gain_attn, gain_ffn = ins
    branch_out, hidden_out = outs
    hidden = tokens[i].astype(F32) + branch * inverse_rms(branch) * gain_attn[...]
    branch_out[i] = branch
    hidden_out[i] = hidden
    return (hidden * inverse_rms(hidden) * gain_ffn[...]).astype(BF16), None


@with_sums(1)
def body_turn(i, branch, ins, outs):
    hidden, upstream, gain = ins
    scale = inverse_rms(branch)
    outs[0][i] = (hidden[i] + branch * scale * gain[...]).astype(BF16)
    grad, term = norm_back(upstream[i].astype(F32), branch, scale, gain[...])
    return grad.astype(BF16), (term,)


@with_sums(2)
def body_back(i, delta, ins, outs):
    hidden, branch, upstream, gain_attn, gain_ffn = ins
    hid, y1 = hidden[i], branch[i]
    part, term_ffn = norm_back(delta, hid, inverse_rms(hid), gain_ffn[...])
    hid_grad = upstream[i].astype(F32) + part
    outs[0][i] = hid_grad
    grad, term_attn = norm_back(hid_grad, y1, inverse_rms(y1), gain_attn[...])
    return grad.astype(BF16), (term_ffn, term_attn)


@with_sums(1)
def body_last(i, delta, ins, outs):
    tokens, hidden_grad, gain = ins
    values = tokens[i].astype(F32)
    part, term = norm_back(delta, values, inverse_rms(values), gain[...])
    outs[0][i] = (hidden_grad[i] + part).astype(BF16)
    return None, (term,)


def scores(q, k):
    s = jnp.einsum("bqd,bkd->bqk", q, k, preferred_element_type=F32) * QUERY_FACTOR
    t = jnp.tanh(s / SOFT_CAP)
    length = q.shape[1]
    allowed = jnp.arange(length)[None, :] <= jnp.arange(length)[:, None]
    return t, jnp.where(allowed[None], SOFT_CAP * t, MASKED)


def attend(q, k, v):
    _, c = scores(q, k)
    top = jnp.max(c, axis=-1, keepdims=True)
    lse = top + jnp.log(jnp.sum(jnp.exp(c - top), axis=-1, keepdims=True))
    p = jnp.exp(c - lse).astype(BF16)
    return jnp.einsum("bqk,bkd->bqd", p, v, preferred_element_type=F32).astype(BF16), lse


def attend_back(q, k, v, o, do, lse):
    t, c = scores(q, k)
    p = jnp.exp(c - lse)
    dd = jnp.sum(do.astype(F32) * o.astype(F32), axis=-1, keepdims=True)
    dp = jnp.einsum("bqd,bkd->bqk", do, v, preferred_element_type=F32)
    ds = (p * (dp - dd) * (1.0 - t * t) * QUERY_FACTOR).astype(BF16)
    dv = jnp.einsum("bqk,bqd->bkd", p.astype(BF16), do, preferred_element_type=F32)
    dk = jnp.einsum("bqk,bqd->bkd", ds, q, preferred_element_type=F32)
    dq = jnp.einsum("bqk,bkd->bqd", ds, k, preferred_element_type=F32)
    return dq.astype(BF16), dk.astype(BF16), dv.astype(BF16)


def dot_f32(a, b):
    return jnp.dot(a, b, preferred_element_type=F32)


def dot_nt(a, b):
    return lax.dot_general(a, b, (((1,), (1,)), ((), ())), preferred_element_type=F32)


def dot_tn(a, b):
    return lax.dot_general(a, b, (((0,), (0,)), ((), ())), preferred_element_type=F32)


def swap(x, axis):
    return lax.all_to_all(x, axis, split_axis=0, concat_axis=0, tiled=True)


def on_device_plane(
    ns, nf,
    tokens, pre_attn_gain, qkv_weight, out_weight, post_attn_gain, pre_ffn_gain,
    gate_up_weight, down_weight, post_ffn_gain, out_grad,
):
    _, chunk, width = tokens.shape
    length = chunk * ns
    spp = nf // ns
    r = chunk // nf
    rows = spp * ns
    group = H // KV
    ff = down_weight.shape[0]
    ffp = -(-ff // LANES) * LANES
    depth = qkv_weight.shape[0]

    both = jnp.stack([tokens[0], out_grad[0]])
    both = both.reshape(2, nf, r, width).transpose(1, 0, 2, 3)
    both = swap(both, "fsdp")
    both = swap(both.reshape(ns, spp * 2 * r, width), "seq")
    both = both.reshape(ns, spp, 2, r, width)
    x_own = both[:, :, 0].transpose(1, 0, 2, 3).reshape(rows, r, width)
    g_own = both[:, :, 1].transpose(1, 0, 2, 3).reshape(rows, r, width)

    q_cols = qkv_weight[:, : H * HD].reshape(depth, H, HD)
    k_cols = jnp.repeat(qkv_weight[:, H * HD : (H + KV) * HD].reshape(depth, KV, HD), group, axis=1)
    v_cols = jnp.repeat(qkv_weight[:, (H + KV) * HD :].reshape(depth, KV, HD), group, axis=1)
    w_qkv = jnp.concatenate([q_cols, k_cols, v_cols], axis=2).transpose(1, 0, 2)
    w_qkv = swap(w_qkv, "fsdp").reshape(nf * depth, 3 * HD)
    w_gu = jnp.pad(gate_up_weight.reshape(depth, 2, nf, ff), ((0, 0), (0, 0), (0, 0), (0, ffp - ff)))
    w_gu = swap(w_gu.transpose(2, 0, 1, 3).reshape(nf, depth, 2 * ffp), "fsdp")
    w_gu = w_gu.reshape(nf * depth, 2 * ffp)
    w_down = jnp.pad(down_weight, ((0, ffp - ff), (0, 0)))

    gains = [g.reshape(1, width) for g in (pre_attn_gain, post_attn_gain, pre_ffn_gain, post_ffn_gain)]
    flat = (rows * nf * r, width)
    terms = (rows, nf, r, width)

    a_full, = plane_call("gather_a", 1, body_first, None, [x_own, gains[0]], [], True, nf, width)
    a_full = a_full.reshape(flat)
    qkv = dot_f32(a_full, w_qkv).astype(BF16)
    q, k, v = (qkv[:, i * HD : (i + 1) * HD].reshape(spp, length, HD) for i in range(3))
    o, lse = attend(q, k, v)
    o_flat = o.reshape(-1, HD)
    y1_terms = dot_f32(o_flat, out_weight).astype(BF16).reshape(terms)
    n_full, y1, hidden = plane_call(
        "mid", 2, body_mid, y1_terms, [x_own, gains[1], gains[2]], [F32, F32], True, nf, width
    )
    n_full = n_full.reshape(flat)
    gu = dot_f32(n_full, w_gu)
    gate, up = gu[:, :ffp], gu[:, ffp:]
    activated, derivative = gelu_pair(gate)
    mixed = (activated * up).astype(BF16)
    y2_terms = dot_f32(mixed, w_down).astype(BF16).reshape(terms)
    dy2_full, out_own, post_ffn_term = plane_call(
        "turn", 3, body_turn, y2_terms, [hidden, g_own, gains[3]], [BF16], True, nf, width
    )
    dy2_full = dy2_full.reshape(flat)
    down_wg = dot_tn(mixed, dy2_full)[:ff].astype(BF16)
    down_wg = lax.psum(down_wg, "seq")
    dm = dot_nt(dy2_full, w_down)
    dgu = jnp.concatenate([dm * up * derivative, dm * activated], axis=1).astype(BF16)
    dn_terms = dot_nt(dgu, w_gu).astype(BF16).reshape(terms)
    gu_wg = dot_tn(n_full, dgu).astype(BF16).reshape(nf, depth, 2 * ffp)
    gu_wg = swap(gu_wg, "fsdp").reshape(nf, depth, 2, ffp)[..., :ff]
    gu_wg = lax.psum(gu_wg.transpose(1, 2, 0, 3).reshape(depth, 2 * nf * ff), "seq")
    dy1_full, hidden_grad, pre_ffn_term, post_attn_term = plane_call(
        "back", 4, body_back, dn_terms, [hidden, y1, g_own, gains[1], gains[2]], [F32], True, nf, width
    )
    dy1_full = dy1_full.reshape(flat)
    do = dot_nt(dy1_full, out_weight).astype(BF16).reshape(o.shape)
    out_wg = dot_tn(o_flat, dy1_full).astype(BF16)
    dq, dk, dv = attend_back(q, k, v, o, do, lse)
    dqkv = jnp.concatenate([dq, dk, dv], axis=2).reshape(-1, 3 * HD)
    da_terms = dot_nt(dqkv, w_qkv).astype(BF16).reshape(terms)
    qkv_wg = dot_tn(a_full, dqkv).astype(BF16).reshape(nf, depth, 3 * HD)
    qkv_wg = swap(qkv_wg, "fsdp").transpose(1, 0, 2)
    kv_wg = qkv_wg[:, :, HD:].astype(F32).reshape(depth, KV, group, 2 * HD).sum(axis=2).astype(BF16)
    qkv_wg = jnp.concatenate(
        [
            qkv_wg[:, :, :HD].reshape(depth, H * HD),
            kv_wg[:, :, :HD].reshape(depth, KV * HD),
            kv_wg[:, :, HD:].reshape(depth, KV * HD),
        ],
        axis=1,
    )
    out_wg, qkv_wg = lax.psum((out_wg, qkv_wg), "seq")
    tg_own, pre_attn_term = plane_call(
        "last", 5, body_last, da_terms, [x_own, hidden_grad, gains[0]], [BF16], False, nf, width
    )
    back = jnp.stack([out_own, tg_own], axis=2)
    back = jnp.stack([out_own, tg_own]).reshape(2, spp, ns, r, width).transpose(2, 1, 0, 3, 4)
    back = swap(back.reshape(ns, spp * 2 * r, width), "seq").reshape(nf, 2, r, width)
    back = swap(back, "fsdp").transpose(1, 0, 2, 3).reshape(2, 1, chunk, width)
    gain_sums = lax.psum(
        jnp.concatenate([pre_attn_term, post_attn_term, pre_ffn_term, post_ffn_term]), ("seq", "fsdp")
    )
    return (
        back[0],
        back[1].astype(F32),
        gain_sums[0],
        qkv_wg.astype(F32),
        out_wg.astype(F32),
        gain_sums[1],
        gain_sums[2],
        gu_wg.astype(F32),
        down_wg.astype(F32),
        gain_sums[3],
    )


def gathered_norm_back(upstream, values, inv_scale, gains):
    weighted = upstream * gains
    inner_mean = jnp.mean(weighted * values, axis=-1, keepdims=True)
    gradient = inv_scale * weighted - values * (inv_scale * inv_scale * inv_scale) * inner_mean
    gain_grad = jnp.sum(upstream * values * inv_scale, axis=0)
    return (gradient, gain_grad)


def batched_contraction(pattern, left_side, right_side):
    return jnp.einsum(pattern, left_side, right_side, preferred_element_type=jnp.float32)


def gathered_capped_scores(block_of_queries, key_row_slices, offset):
    amount = block_of_queries.shape[0]
    key_count = key_row_slices.shape[0]
    unscaled_logits = (
        batched_contraction("olv,ilv->loi", block_of_queries, key_row_slices) * QUERY_FACTOR
    )
    tanh_part = jnp.tanh(unscaled_logits / SOFT_CAP)
    allowed = (
        jnp.arange(key_count, dtype=jnp.int32)[None, :]
        <= (offset + jnp.arange(amount, dtype=jnp.int32))[:, None]
    )
    capped = jnp.where(allowed[None], SOFT_CAP * tanh_part, MASKED)
    return (tanh_part, capped)


def gathered_attend(queries, key_row_slices, value_row_slices):
    length = queries.shape[0]
    block_size = min(512, length)
    blocks = length // block_size

    def one_block(block_id):
        offset = block_id * block_size
        block_of_queries = lax.dynamic_slice_in_dim(queries, offset, block_size, 0)
        tanh_part, capped = gathered_capped_scores(block_of_queries, key_row_slices, offset)
        biggest = jnp.max(capped, axis=-1, keepdims=True)
        logsum = biggest + jnp.log(jnp.sum(jnp.exp(capped - biggest), axis=-1, keepdims=True))
        attention_probabilities = jnp.exp(capped - logsum).astype(jnp.bfloat16)
        layer_result = batched_contraction(
            "vxn,nvs->xvs", attention_probabilities, value_row_slices
        ).astype(jnp.bfloat16)
        return (layer_result, logsum[..., 0])

    outputs, logsums = lax.map(one_block, jnp.arange(blocks, dtype=jnp.int32))
    return (outputs.reshape(queries.shape), logsums)


def gathered_attend_back(queries, key_row_slices, value_row_slices, outputs, out_delta, logsums):
    length = queries.shape[0]
    block_size = min(512, length)
    blocks = length // block_size
    row_dots = batched_contraction("qbd,qbd->bq", out_delta, outputs)

    def one_block(carried, inputs):
        key_accumulator, value_accumulator = carried
        block_id, block_logsum = inputs
        offset = block_id * block_size
        block_of_queries = lax.dynamic_slice_in_dim(queries, offset, block_size, 0)
        block_correction = lax.dynamic_slice_in_dim(out_delta, offset, block_size, 0)
        tanh_part, capped = gathered_capped_scores(block_of_queries, key_row_slices, offset)
        attention_probabilities = jnp.exp(capped - block_logsum[..., None])
        probability_gradients = batched_contraction(
            "olv,ilv->loi", block_correction, value_row_slices
        )
        dots_block = lax.dynamic_slice_in_dim(row_dots, offset, block_size, 1)
        logit_gradients = (
            attention_probabilities
            * (probability_gradients - dots_block[..., None])
            * (1.0 - tanh_part * tanh_part)
            * QUERY_FACTOR
        ).astype(jnp.bfloat16)
        rounded_values = attention_probabilities.astype(jnp.bfloat16)
        value_accumulator = value_accumulator + batched_contraction(
            "pfm,fpg->mpg", rounded_values, block_correction
        )
        key_accumulator = key_accumulator + batched_contraction(
            "pfm,fpg->mpg", logit_gradients, block_of_queries
        )
        query_gradient = batched_contraction(
            "vxn,nvs->xvs", logit_gradients, key_row_slices
        ).astype(jnp.bfloat16)
        return ((key_accumulator, value_accumulator), query_gradient)

    zero_acc = jnp.zeros(key_row_slices.shape, jnp.float32)
    (key_accumulator, value_accumulator), query_grads = lax.scan(
        one_block, (zero_acc, zero_acc), (jnp.arange(blocks, dtype=jnp.int32), logsums)
    )
    return (
        query_grads.reshape(queries.shape),
        key_accumulator.astype(jnp.bfloat16),
        value_accumulator.astype(jnp.bfloat16),
    )


def gathered_project(activations, weight_shard):
    return jnp.dot(
        activations,
        lax.all_gather(weight_shard, "fsdp", axis=0, tiled=True),
        preferred_element_type=jnp.float32,
    )


def gathered_project_back(gradient, weight_shard):
    return lax.dot_general(
        gradient,
        lax.all_gather(weight_shard, "fsdp", axis=0, tiled=True),
        (((1,), (1,)), ((), ())),
        preferred_element_type=jnp.float32,
    )


def term_maker(activations, gradient):
    return lax.dot_general(
        activations, gradient, (((0,), (0,)), ((), ())), preferred_element_type=jnp.float32
    )


def weight_term(activations, gradient):
    sliced = lax.psum_scatter(
        term_maker(activations, gradient).astype(jnp.bfloat16),
        "fsdp",
        scatter_dimension=0,
        tiled=True,
    )
    return lax.psum(sliced, "seq").astype(jnp.float32)


def gathered_on_device(
    tokens,
    pre_attn_gain,
    qkv_weight,
    out_weight,
    post_attn_gain,
    pre_ffn_gain,
    gate_up_weight,
    down_weight,
    post_ffn_gain,
    out_grad,
):
    groups, local_len, width = tokens.shape
    row_count = groups * local_len
    head_repeat = H // KV
    ff = gate_up_weight.shape[1] // 2
    residual_in = tokens.reshape(row_count, width).astype(jnp.float32)
    scale_one = inverse_rms(residual_in)
    normed_in = (residual_in * scale_one * pre_attn_gain).astype(jnp.bfloat16)
    projected = gathered_project(normed_in, qkv_weight).astype(jnp.bfloat16)
    queries = projected[:, : H * HD].reshape(groups, local_len, H, HD)
    key_row_slices = jnp.repeat(
        projected[:, H * HD : (H + KV) * HD].reshape(groups, local_len, KV, HD), head_repeat, axis=2
    )
    value_row_slices = jnp.repeat(
        projected[:, (H + KV) * HD :].reshape(groups, local_len, KV, HD), head_repeat, axis=2
    )
    head_queries, head_keys, head_values = (
        lax.all_to_all(queries, "seq", split_axis=2, concat_axis=1, tiled=True),
        lax.all_to_all(key_row_slices, "seq", split_axis=2, concat_axis=1, tiled=True),
        lax.all_to_all(value_row_slices, "seq", split_axis=2, concat_axis=1, tiled=True),
    )
    head_out, logsums = jax.vmap(gathered_attend)(head_queries, head_keys, head_values)
    attn_out = lax.all_to_all(head_out, "seq", split_axis=1, concat_axis=2, tiled=True).reshape(
        row_count, H * HD
    )
    branch_one = gathered_project(attn_out, out_weight)
    scale_two = inverse_rms(branch_one)
    hidden = residual_in + branch_one * scale_two * post_attn_gain
    scale_three = inverse_rms(hidden)
    normed_mid = (hidden * scale_three * pre_ffn_gain).astype(jnp.bfloat16)
    gate_up = gathered_project(normed_mid, gate_up_weight)
    gate_part = gate_up[:, :ff]
    up_part = gate_up[:, ff:]
    activated, derivative = gelu_pair(gate_part)
    mixed = (activated * up_part).astype(jnp.bfloat16)
    branch_two = gathered_project(mixed, down_weight)
    scale_four = inverse_rms(branch_two)
    layer_out = (
        (hidden + branch_two * scale_four * post_ffn_gain)
        .astype(jnp.bfloat16)
        .reshape(groups, local_len, width)
    )
    upstream = out_grad.reshape(row_count, width).astype(jnp.float32)
    branch_two_grad, post_ffn_term = gathered_norm_back(upstream, branch_two, scale_four, post_ffn_gain)
    branch_two_grad = branch_two_grad.astype(jnp.bfloat16)
    down_wgrad = weight_term(mixed, branch_two_grad)
    mixed_grad = gathered_project_back(branch_two_grad, down_weight)
    gate_up_grad = jnp.concatenate(
        [mixed_grad * up_part * derivative, mixed_grad * activated], axis=1
    ).astype(jnp.bfloat16)
    gate_up_wgrad = weight_term(normed_mid, gate_up_grad)
    normed_mid_grad = gathered_project_back(gate_up_grad, gate_up_weight)
    hidden_part, pre_ffn_term = gathered_norm_back(normed_mid_grad, hidden, scale_three, pre_ffn_gain)
    hidden_grad = upstream + hidden_part
    branch_one_grad, post_attn_term = gathered_norm_back(hidden_grad, branch_one, scale_two, post_attn_gain)
    branch_one_grad = branch_one_grad.astype(jnp.bfloat16)
    out_wgrad = weight_term(attn_out, branch_one_grad)
    attn_grad = (
        gathered_project_back(branch_one_grad, out_weight)
        .astype(jnp.bfloat16)
        .reshape(groups, local_len, H, HD)
    )
    head_delta = lax.all_to_all(attn_grad, "seq", split_axis=2, concat_axis=1, tiled=True)
    query_gradient, key_grad, value_grad = jax.vmap(gathered_attend_back)(
        head_queries, head_keys, head_values, head_out, head_delta, logsums
    )
    query_tok, key_tok, value_tok = (
        lax.all_to_all(query_gradient, "seq", split_axis=1, concat_axis=2, tiled=True),
        lax.all_to_all(key_grad, "seq", split_axis=1, concat_axis=2, tiled=True),
        lax.all_to_all(value_grad, "seq", split_axis=1, concat_axis=2, tiled=True),
    )
    key_sum = (
        key_tok.astype(jnp.float32)
        .reshape(groups, local_len, KV, head_repeat, HD)
        .sum(axis=3)
        .astype(jnp.bfloat16)
    )
    value_sum = (
        value_tok.astype(jnp.float32)
        .reshape(groups, local_len, KV, head_repeat, HD)
        .sum(axis=3)
        .astype(jnp.bfloat16)
    )
    qkv_grad = jnp.concatenate(
        [
            query_tok.reshape(row_count, H * HD),
            key_sum.reshape(row_count, KV * HD),
            value_sum.reshape(row_count, KV * HD),
        ],
        axis=1,
    )
    qkv_wgrad = weight_term(normed_in, qkv_grad)
    normed_in_grad = gathered_project_back(qkv_grad, qkv_weight)
    input_part, pre_attn_term = gathered_norm_back(normed_in_grad, residual_in, scale_one, pre_attn_gain)
    tokens_grad = (hidden_grad + input_part).reshape(groups, local_len, width)
    gain_sums = lax.psum(
        (pre_attn_term, post_attn_term, pre_ffn_term, post_ffn_term), ("seq", "fsdp")
    )
    return (
        layer_out,
        tokens_grad,
        gain_sums[0],
        qkv_wgrad,
        out_wgrad,
        gain_sums[1],
        gain_sums[2],
        gate_up_wgrad,
        down_wgrad,
        gain_sums[3],
    )


def solution(mesh):
    ns, nf = mesh.shape["seq"], mesh.shape["fsdp"]
    token_spec, row_spec = P("fsdp", "seq", None), P("fsdp", None)
    in_specs = (
        token_spec, P(), row_spec, row_spec, P(), P(), row_spec, row_spec, P(), token_spec,
    )
    out_specs = (
        token_spec, token_spec, P(), row_spec, row_spec, P(), P(), row_spec, row_spec, P(),
    )

    def on_device(*args):
        if nf == 8 and nf == H and nf % ns == 0 and args[0].shape[0] == 1:
            return on_device_plane(ns, nf, *args)
        return gathered_on_device(*args)

    return jax.shard_map(
        on_device, mesh=mesh, in_specs=in_specs, out_specs=out_specs, check_vma=False
    )
```

```python
import functools
import math

import jax
import jax.numpy as jnp
from jax import lax
from jax.experimental import pallas as pl
from jax.experimental.pallas import tpu as pltpu
from jax.sharding import PartitionSpec as P

H = 8
KV = 4
HD = 256

EPSILON = 1e-06
SOFT_CAP = 50.0
QUERY_FACTOR = 0.0625
GELU_COEFF = math.sqrt(2.0 / math.pi)
CUBIC = 0.044715
MASKED = -1e30
MESH = pl.DeviceIdType.MESH
F32 = jnp.float32
BF16 = jnp.bfloat16
LANES = 128


def inverse_rms(values):
    return lax.rsqrt(jnp.mean(values * values, axis=-1, keepdims=True) + EPSILON)


def norm_back(upstream, values, inv_scale, gains):
    weighted = upstream * gains
    inner_mean = jnp.mean(weighted * values, axis=-1, keepdims=True)
    gradient = inv_scale * weighted - values * (inv_scale * inv_scale * inv_scale) * inner_mean
    gain_grad = jnp.sum(upstream * values * inv_scale, axis=0, keepdims=True)
    return (gradient, gain_grad)


def gelu_pair(values):
    inner_part = GELU_COEFF * (values + CUBIC * values * values * values)
    tanh_part = jnp.tanh(inner_part)
    activated = 0.5 * values * (1.0 + tanh_part)
    derivative = 0.5 * (1.0 + tanh_part) + 0.5 * values * (
        1.0 - tanh_part * tanh_part
    ) * GELU_COEFF * (1.0 + 3.0 * CUBIC * values * values)
    return (activated, derivative)


class Place:
    def __init__(self, nf, ns):
        self.nf, self.ns = nf, ns
        self.me, self.z = lax.axis_index("fsdp"), lax.axis_index("seq")
        core, xpos, ypos = self.me % 2, (self.me // 2) % 2, self.me // 4
        self.step = 1 - 2 * core
        self.mate = self.me + self.step
        self.xn = self.me + 2 - 4 * xpos
        self.yn = self.me + 4 - 8 * ypos
        self.diag = self.xn + 4 - 8 * ypos

    def plane_peers(self):
        return [(self.me + d) % self.nf for d in range(1, self.nf)]

    def line_peers(self):
        return [(self.z + d) % self.ns for d in range(1, self.ns)]

    def greet(self, near, plane, line):
        barrier = pltpu.get_barrier_semaphore()
        to = [{"fsdp": p} for p in (self.plane_peers() if plane else (self.mate, self.xn, self.yn) if near else ())]
        to += [{"seq": p} for p in (self.line_peers() if line else ())]
        for device in to:
            pl.semaphore_signal(barrier, inc=1, device_id=device, device_id_type=MESH)
        pl.semaphore_wait(barrier, len(to))


class Wire:
    def __init__(self, lsem, ssem, rsem):
        self.lsem, self.ssem, self.rsem = lsem, ssem, rsem
        self.sent, self.kept = [], []

    def send(self, src, dst, device):
        k = len(self.sent)
        copy = pltpu.make_async_remote_copy(
            src_ref=src, dst_ref=dst, send_sem=self.ssem.at[k], recv_sem=self.rsem.at[k],
            device_id=device, device_id_type=MESH,
        )
        copy.start()
        self.sent.append(copy)
        return copy

    def near(self, src, dst, to):
        return self.send(src, dst, {"fsdp": to})

    def keep(self, src, dst):
        copy = pltpu.make_async_copy(src, dst, self.lsem.at[len(self.kept)])
        copy.start()
        self.kept.append(copy)
        return copy

    def flush(self):
        for copy in self.sent:
            copy.wait_send()


def each(count, f):
    def one(i, _):
        f(i)
        return 0

    lax.fori_loop(0, count, one, 0)


def halves_of(rows):
    return pl.ds(0, rows // 2), pl.ds(rows // 2, rows // 2)


def reduce_start(at, wire, part, acc, other):
    order = (at.diag, at.xn, at.yn, at.me)
    return [wire.keep(part.at[:, b], acc.at[k]) for k, b in enumerate(order)]


def reduce_in_plane(at, wire, own, part, acc, other, ra, rb, rx, ry):
    rows = acc.shape[1]
    half = rows // 2
    h0, h1 = halves_of(rows)
    order = (at.diag, at.xn, at.yn, at.me)
    mates = [wire.near(part.at[:, b + at.step], other.at[k], at.mate) for k, b in enumerate(order)]
    yield

    def add(dst, src, lo, count):
        def one(i):
            dst[lo + i] = (dst[lo + i].astype(F32) + src[i].astype(F32)).astype(BF16)

        each(count, one)

    def join(k):
        own[k].wait()
        mates[k].wait_recv()
        add(acc.at[k], other.at[k], 0, rows)

    join(0)
    ca = wire.near(acc.at[0, h0], ra, at.yn)
    cb = wire.near(acc.at[0, h1], rb, at.xn)
    yield
    join(1)
    cx1 = wire.near(acc.at[1, h1], rx.at[h1], at.xn)
    join(2)
    cy0 = wire.near(acc.at[2, h0], ry.at[h0], at.yn)
    yield
    ca.wait_recv()
    add(acc.at[1], ra, 0, half)
    cx0 = wire.near(acc.at[1, h0], rx.at[h0], at.xn)
    cb.wait_recv()
    add(acc.at[2], rb, half, half)
    cy1 = wire.near(acc.at[2, h1], ry.at[h1], at.yn)
    own[3].wait()
    mates[3].wait_recv()
    yield
    cx1.wait_recv()
    cy0.wait_recv()
    yield
    cx0.wait_recv()
    cy1.wait_recv()


def gather_in_plane(at, wire, block, full):
    h0, h1 = halves_of(block.shape[0])
    me, xn, yn, diag, mate = at.me, at.xn, at.yn, at.diag, at.mate
    keep = wire.keep(block, full.at[:, me])

    def pass_on(copy, where, blk, to):
        copy.wait_recv()
        return wire.near(full.at[where, blk], full.at[where, blk], to)

    y0 = wire.near(block.at[h0], full.at[h0, me], yn)
    x1 = wire.near(block.at[h1], full.at[h1, me], xn)
    y1 = wire.near(block.at[h1], full.at[h1, me], yn)
    x0 = wire.near(block.at[h0], full.at[h0, me], xn)
    last = [wire.near(block, full.at[:, me], mate)]
    yield
    gx = pass_on(y0, h0, yn, xn)
    last.append(wire.near(full.at[h0, yn], full.at[h0, yn], mate))
    gy = pass_on(x1, h1, xn, yn)
    last.append(wire.near(full.at[h1, xn], full.at[h1, xn], mate))
    yield
    last.append(pass_on(y1, h1, yn, mate))
    last.append(pass_on(x0, h0, xn, mate))
    yield
    last.append(pass_on(gx, h0, diag, mate))
    last.append(pass_on(gy, h1, diag, mate))
    yield
    for copy in last:
        copy.wait_recv()
    keep.wait()


def weave(main, others=(), counts=()):
    others, counts = list(others), list(counts)
    for _ in main:
        for _ in range(counts.pop(0) if counts else 0):
            if others:
                others.pop(0)()
    for other in others:
        other()


class LineSum:
    def __init__(self, at, items, sems):
        self.z, self.items, self.sems = at.z, items, sems
        self.outer = at.z % 3 == 0
        self.inner = at.z % 3 != 0
        self.pair = at.z + 1 - 2 * (at.z % 2)
        self.across = 3 - at.z

    def copy(self, stage, k):
        own, in1, in2, out = self.items[k]
        src, dst, to = ((own, in1, self.pair), (in1, in2, self.across), (in2, out, self.pair))[stage]
        send, recv = self.sems[2 * stage], self.sems[2 * stage + 1]
        return pltpu.make_async_remote_copy(
            src_ref=src, dst_ref=dst, send_sem=send.at[k], recv_sem=recv.at[k],
            device_id={"seq": to}, device_id_type=MESH,
        )

    def kept(self, k):
        return pltpu.make_async_copy(self.items[k][2], self.items[k][3], self.sems[6].at[k])

    @staticmethod
    def add(dst, src):
        def one(i):
            where = pl.ds(pl.multiple_of(i * 16, 16), 16)
            dst[where] = (dst[where].astype(F32) + src[where].astype(F32)).astype(BF16)

        each(dst.shape[0] // 16, one)

    def launch(self, k):
        @pl.when(self.outer)
        def _():
            self.copy(0, k).start()

    def first(self, k):
        @pl.when(self.inner)
        def _():
            self.copy(0, k).wait_recv()
            self.add(self.items[k][1], self.items[k][0])
            self.copy(1, k).start()

    def second(self, k):
        @pl.when(self.inner)
        def _():
            self.copy(1, k).wait_recv()
            self.add(self.items[k][2], self.items[k][1])
            self.copy(2, k).start()
            self.kept(k).start()

    def steps(self):
        n = len(self.items)
        out = []
        for k in range(n + 1):
            if k < n:
                out.append(functools.partial(self.first, k))
            if k > 0:
                out.append(functools.partial(self.second, k - 1))
        return out

    def end(self):
        for k in range(len(self.items)):

            @pl.when(self.outer)
            def _():
                self.copy(0, k).wait_send()
                self.copy(2, k).wait_recv()

            @pl.when(self.inner)
            def _():
                self.copy(1, k).wait_send()
                self.copy(2, k).wait_send()
                self.kept(k).wait()

    @staticmethod
    def semaphores(n):
        return [pltpu.SemaphoreType.DMA((n,))] * 7


def enter_kernel(nf, ns, tok, grad, gain, full, x_own, g_own, xs, gs, xo, go, block, lsem, ssem, rsem):
    at, wire = Place(nf, ns), Wire(lsem, ssem, rsem)
    keeps = [wire.keep(tok.at[at.me], xs.at[at.me]), wire.keep(grad.at[at.me], gs.at[at.me])]
    at.greet(True, True, True)
    first = [
        [wire.near(src.at[p], dst.at[at.me], p) for p in at.plane_peers()]
        for src, dst in ((tok, xs), (grad, gs))
    ]
    spp = nf // ns
    second, own = [], []
    for k, (src, dst) in enumerate(((xs, xo), (gs, go))):
        keeps[k].wait()
        for copy in first[k]:
            copy.wait_recv()
        second.append(
            [
                wire.send(src.at[pl.ds(p * spp, spp)], dst.at[:, at.z], {"seq": p})
                for p in at.line_peers()
            ]
        )
        own.append(wire.keep(src.at[pl.ds(at.z * spp, spp)], dst.at[:, at.z]))
    own[0].wait()
    for copy in second[0]:
        copy.wait_recv()
    outs = [wire.keep(xo, x_own)]

    def one(i):
        values = xo[i // ns, i % ns].astype(F32)
        block[i] = (values * inverse_rms(values) * gain[...]).astype(BF16)

    each(nf, one)
    weave(gather_in_plane(at, wire, block, full))
    own[1].wait()
    for copy in second[1]:
        copy.wait_recv()
    outs.append(wire.keep(go, g_own))
    for copy in outs:
        copy.wait()
    wire.flush()


def enter(nf, ns, tokens, grads, gain):
    _, r, width = tokens.shape
    spp = nf // ns
    own = jax.ShapeDtypeStruct((spp, ns, r, width), BF16)
    anys = pl.BlockSpec(memory_space=pl.ANY)
    n_send = 2 * (nf - 1) + 2 * (ns - 1) + 13
    return pl.pallas_call(
        functools.partial(enter_kernel, nf, ns),
        name="enter",
        out_shape=[jax.ShapeDtypeStruct((nf, nf, r, width), BF16), own, own],
        in_specs=[anys, anys, pl.BlockSpec(memory_space=pltpu.VMEM)],
        out_specs=[anys, anys, anys],
        scratch_shapes=[pltpu.VMEM((nf, r, width), BF16)] * 2
        + [pltpu.VMEM((spp, ns, r, width), BF16)] * 2
        + [pltpu.VMEM((nf, r, width), BF16)]
        + [pltpu.SemaphoreType.DMA((8,))]
        + [pltpu.SemaphoreType.DMA((n_send,))] * 2,
        compiler_params=pltpu.CompilerParams(collective_id=1, has_side_effects=True),
    )(tokens, grads, gain)


def middle_kernel(nf, ns, n_in, n_own, body, plan, *refs):
    refs = list(refs)
    part, ins = refs[0], refs[1 : 1 + n_in]
    del refs[: 1 + n_in]
    grad = refs.pop(0) if plan else None
    full = refs.pop(0)
    outs = [refs.pop(0) for _ in range(n_own)]
    summed = refs.pop(0) if plan else None
    acc, other, ra, rb, rx, ry, block, lsem, ssem, rsem = refs[:10]
    at, wire = Place(nf, ns), Wire(lsem, ssem, rsem)
    own = reduce_start(at, wire, part, acc, other)
    at.greet(True, False, plan)
    line, steps = None, ()
    if plan:
        in1, in2 = refs[10:12]
        line = LineSum(at, [(grad.at[k], in1.at[k], in2.at[k], summed.at[k]) for k in range(grad.shape[0])], refs[12:])

    def main():
        yield from reduce_in_plane(at, wire, own, part, acc, other, ra, rb, rx, ry)
        work_on_sum(body, acc, other, rx, ry, ins, outs, block)
        yield from gather_in_plane(at, wire, block, full)

    if plan:
        for k in range(len(line.items)):
            line.launch(k)
        weave(main(), line.steps(), plan)
        line.end()
    else:
        weave(main())
    wire.flush()


def work_on_sum(body, acc, other, rx, ry, ins, outs, block):
    def one(i, sums):
        total = (acc[3, i].astype(F32) + other[3, i].astype(F32)) + (
            rx[i].astype(F32) + ry[i].astype(F32)
        )
        block[i], extra = body(i, total, ins, outs)
        return tuple(s + e for s, e in zip(sums, extra))

    rows, _, width = block.shape
    zero = tuple(jnp.zeros((1, width), F32) for _ in range(body.n_sums))
    sums = lax.fori_loop(0, rows, one, zero)
    for s, ref in zip(sums, outs[len(outs) - body.n_sums :]):
        ref[...] = s


def sum_scratch(rows, r, width):
    shape, half = (rows, r, width), (rows // 2, r, width)
    return [pltpu.VMEM((4,) + shape, BF16)] * 2 + [pltpu.VMEM(half, BF16)] * 2 + [pltpu.VMEM(shape, BF16)] * 3


def middle(name, cid, nf, ns, body, part, ins, own_types, grad=None, plan=None):
    rows, _, r, width = part.shape
    vmem, anys = pl.BlockSpec(memory_space=pltpu.VMEM), pl.BlockSpec(memory_space=pl.ANY)
    out_shape = [jax.ShapeDtypeStruct(part.shape, BF16)]
    out_shape += [jax.ShapeDtypeStruct((rows, r, width), t) for t in own_types]
    out_shape += [jax.ShapeDtypeStruct((1, width), F32)] * body.n_sums
    n_own = len(out_shape) - 1
    in_specs, out_specs = [anys] + [vmem] * len(ins), [anys] + [vmem] * n_own
    scratch = sum_scratch(rows, r, width)
    scratch += [pltpu.SemaphoreType.DMA((5,))] + [pltpu.SemaphoreType.DMA((23,))] * 2
    operands = [part, *ins]
    if plan:
        operands.append(grad)
        in_specs.append(vmem)
        out_shape.append(jax.ShapeDtypeStruct(grad.shape, BF16))
        out_specs.append(anys)
        scratch += [pltpu.VMEM(grad.shape, BF16)] * 2 + LineSum.semaphores(grad.shape[0])
    return pl.pallas_call(
        functools.partial(middle_kernel, nf, ns, len(ins), n_own, body, plan),
        name=name,
        out_shape=out_shape,
        in_specs=in_specs,
        out_specs=out_specs,
        scratch_shapes=scratch,
        compiler_params=pltpu.CompilerParams(collective_id=cid, has_side_effects=True),
    )(*operands)


def leave_kernel(nf, ns, body, *refs):
    part, tokens, hid_grad, gain, done, terms, gu, qkv, wout = refs[:9]
    lay_out, tok_out, gain_out, gu_out, qkv_out, wout_out = refs[9:15]
    (acc, other, ra, rb, rx, ry, block, dz, bz, gl, gt, gp, gz, gu_in, gu1, gu2,
     qkv_in, qkv_own, qkv1, qkv2, w1, w2) = refs[15:37]
    lsem, ssem, rsem = refs[37:40]
    zsems = refs[40:]
    at, wire = Place(nf, ns), Wire(lsem, ssem, rsem)
    spp = nf // ns
    own = reduce_start(at, wire, part, acc, other)
    own_dz = wire.keep(done.at[:, at.z], dz.at[pl.ds(at.z * spp, spp)])
    own_gu = wire.keep(gu.at[at.me], gu_in.at[at.me])
    own_qkv = wire.keep(qkv.at[at.me], qkv_in.at[at.me])
    at.greet(True, True, True)

    half = gu_in.shape[2] // 2
    order = (at.me, at.mate, at.xn, at.yn, at.xn + at.step, at.yn + at.step, at.diag, at.diag + at.step)
    items = [(wout.at[k], w1.at[k], w2.at[k], wout_out.at[k]) for k in range(wout.shape[0])]
    n_out = len(items)
    for p in order:
        for h in range(2):
            where = (p, slice(None), pl.ds(h * half, half))
            items.append(tuple(ref.at[where] for ref in (gu_in, gu1, gu2, gu_out)))
    for c in range(qkv_own.shape[0]):
        items.append(tuple(ref.at[c] for ref in (qkv_own, qkv1, qkv2, qkv_out)))
    line = LineSum(at, items, zsems)
    for k in range(n_out):
        line.launch(k)

    main = reduce_in_plane(at, wire, own, part, acc, other, ra, rb, rx, ry)
    next(main)
    gu_moves = {1: wire.near(gu.at[at.mate], gu_in.at[at.me], at.mate)}
    for j in range(2, nf):
        gu_moves[j] = wire.near(gu.at[order[j]], gu_in.at[at.me], order[j])
    qkv_moves = [wire.near(qkv.at[p], qkv_in.at[at.me], p) for p in at.plane_peers()]
    lay = [
        wire.send(done.at[:, p], dz.at[pl.ds(at.z * spp, spp)], {"seq": p}) for p in at.line_peers()
    ]

    def arrive(j):
        if j == 0:
            own_gu.wait()
        else:
            gu_moves[j].wait_recv()
        line.launch(n_out + 2 * j)
        line.launch(n_out + 2 * j + 1)

    def arrive_qkv():
        own_qkv.wait()
        for copy in qkv_moves:
            copy.wait_recv()
        group = nf // qkv_own.shape[0]
        hd = HD

        def one(i):
            where = pl.ds(pl.multiple_of(i * 16, 16), 16)
            for c in range(qkv_own.shape[0]):
                both = jnp.zeros((16, 2 * hd), F32)
                for g in range(group):
                    piece = qkv_in[c * group + g, where]
                    qkv_own[c, where, g * hd : (g + 1) * hd] = piece[:, :hd]
                    both = both + piece[:, hd:].astype(F32)
                qkv_own[c, where, group * hd :] = both.astype(BF16)

        each(qkv_own.shape[1] // 16, one)
        for c in range(qkv_own.shape[0]):
            line.launch(n_out + 2 * nf + c)

    def rest():
        yield from main
        gl[...] = terms[...]
        work_on_sum(body, acc, other, rx, ry, (tokens, hid_grad, gain), (gl.at[pl.ds(0, 1)],), block)
        line2, own_bz = [], []
        for s in range(spp):
            own_bz.append(wire.keep(block.at[s * ns + at.z], bz.at[at.z * spp + s]))
            line2 += [
                wire.send(block.at[s * ns + p], bz.at[at.z * spp + s], {"seq": p})
                for p in at.line_peers()
            ]
        gp[at.me] = gl[...]
        small = [wire.near(gl, gp.at[at.me], p) for p in at.plane_peers()]
        yield

        def to_homes(src, out, arrived):
            for copy in arrived:
                copy.wait_recv()
            home = wire.keep(src.at[at.me], out.at[at.me])
            return home, [wire.near(src.at[p], out.at[at.me], p) for p in at.plane_peers()]

        own_dz.wait()
        home1, away1 = to_homes(dz, lay_out, lay)
        yield
        for copy in small:
            copy.wait_recv()
        total = gp[0]
        for k in range(1, nf):
            total = total + gp[k]
        gt[...] = total
        gz[at.z] = total
        small2 = [wire.send(gt, gz.at[at.z], {"seq": p}) for p in at.line_peers()]
        yield
        for copy in own_bz:
            copy.wait()
        home2, away2 = to_homes(bz, tok_out, line2)
        yield
        for copy in small2:
            copy.wait_recv()
        total = gz[0]
        for k in range(1, ns):
            total = total + gz[k]
        gain_out[...] = total
        for copy in away1 + away2:
            copy.wait_recv()
        home1.wait()
        home2.wait()
        yield

    work = [lambda: arrive(0), lambda: arrive(1)]
    steps = line.steps()
    slow = rest()
    ready = {4: 2, 7: 3, 10: 4, 13: 5, 16: 6, 19: 7, 22: None}
    for f in work:
        f()
    for i, step in enumerate(steps):
        step()
        if i in ready:
            arrive_qkv() if ready[i] is None else arrive(ready[i])
        if i % 2 == 1:
            next(slow, None)
    for _ in slow:
        pass
    line.end()
    wire.flush()


def leave(nf, ns, body, part, tokens, hid_grad, gain, done, terms, gu, qkv, wout):
    rows, _, r, width = part.shape
    spp = nf // ns
    depth = gu.shape[1]
    vmem, anys = pl.BlockSpec(memory_space=pltpu.VMEM), pl.BlockSpec(memory_space=pl.ANY)
    home = jax.ShapeDtypeStruct((nf, r, width), BF16)
    n_send = 10 + (ns - 1) * (1 + spp) + (nf - 1) + (ns - 1) + 2 * (nf - 1) + 2 * (nf - 1)
    heads = (KV, depth, (H // KV + 2) * HD)
    n_items = wout.shape[0] + 2 * nf + KV
    return pl.pallas_call(
        functools.partial(leave_kernel, nf, ns, body),
        name="leave",
        out_shape=[home, home, jax.ShapeDtypeStruct((8, width), F32)]
        + [jax.ShapeDtypeStruct(s, BF16) for s in (gu.shape, heads, wout.shape)],
        in_specs=[anys, vmem, vmem, vmem, anys, vmem, anys, anys, vmem],
        out_specs=[anys, anys, vmem, anys, anys, anys],
        scratch_shapes=sum_scratch(rows, r, width)
        + [pltpu.VMEM((nf, r, width), BF16)] * 2
        + [pltpu.VMEM((8, width), F32)] * 2
        + [pltpu.VMEM((nf, 8, width), F32), pltpu.VMEM((ns, 8, width), F32)]
        + [pltpu.VMEM(gu.shape, BF16)] * 3
        + [pltpu.VMEM(qkv.shape, BF16)]
        + [pltpu.VMEM(heads, BF16)] * 3
        + [pltpu.VMEM(wout.shape, BF16)] * 2
        + [pltpu.SemaphoreType.DMA((5 + spp + 4,))]
        + [pltpu.SemaphoreType.DMA((n_send,))] * 2
        + LineSum.semaphores(n_items),
        compiler_params=pltpu.CompilerParams(collective_id=5, has_side_effects=True),
    )(part, tokens, hid_grad, gain, done, terms, gu, qkv, wout)


def split_columns(weight, nf, ff, ffp):
    depth = weight.shape[0]
    step = 16

    def kernel(w, out):
        for f in range(nf):
            for g in range(2):
                piece = w[:, (g * nf + f) * ff : (g * nf + f + 1) * ff]
                if ffp > ff:
                    piece = jnp.concatenate([piece, jnp.zeros((step, ffp - ff), piece.dtype)], axis=1)
                out[f, :, g * ffp : (g + 1) * ffp] = piece

    return pl.pallas_call(
        kernel,
        name="split_columns",
        grid=(depth // step,),
        out_shape=jax.ShapeDtypeStruct((nf, depth, 2 * ffp), weight.dtype),
        in_specs=[pl.BlockSpec((step, 2 * nf * ff), lambda i: (i, 0))],
        out_specs=pl.BlockSpec((nf, step, 2 * ffp), lambda i: (0, i, 0)),
    )(weight)


def join_columns(parts, heads, nf, ff):
    _, depth, columns = parts.shape
    n_kv, _, wide = heads.shape
    queries = wide - 2 * HD
    step = 16

    def kernel(x, h, out, out_h):
        for g in range(2):
            lo = g * columns // 2
            pieces = [x[f, :, lo : lo + ff].astype(F32) for f in range(nf)]
            out[:, g * nf * ff : (g + 1) * nf * ff] = jnp.concatenate(pieces, axis=1)
        for c in range(n_kv):
            piece = h[c].astype(F32)
            out_h[:, c * queries : (c + 1) * queries] = piece[:, :queries]
            for j in range(2):
                lo = n_kv * queries + (j * n_kv + c) * HD
                out_h[:, lo : lo + HD] = piece[:, queries + j * HD : queries + (j + 1) * HD]

    return pl.pallas_call(
        kernel,
        name="join_columns",
        grid=(depth // step,),
        out_shape=[
            jax.ShapeDtypeStruct((depth, 2 * nf * ff), F32),
            jax.ShapeDtypeStruct((depth, n_kv * wide), F32),
        ],
        in_specs=[
            pl.BlockSpec((nf, step, columns), lambda i: (0, i, 0)),
            pl.BlockSpec((n_kv, step, wide), lambda i: (0, i, 0)),
        ],
        out_specs=[
            pl.BlockSpec((step, 2 * nf * ff), lambda i: (i, 0)),
            pl.BlockSpec((step, n_kv * wide), lambda i: (i, 0)),
        ],
    )(parts, heads)


def with_sums(n):
    def mark(f):
        f.n_sums = n
        return f

    return mark


@with_sums(0)
def body_mid(i, branch, ins, outs):
    tokens, gain_attn, gain_ffn = ins
    branch_out, hidden_out = outs
    hidden = tokens[i].astype(F32) + branch * inverse_rms(branch) * gain_attn[...]
    branch_out[i] = branch
    hidden_out[i] = hidden
    return (hidden * inverse_rms(hidden) * gain_ffn[...]).astype(BF16), ()


@with_sums(1)
def body_turn(i, branch, ins, outs):
    hidden, upstream, gain = ins
    scale = inverse_rms(branch)
    outs[0][i] = (hidden[i] + branch * scale * gain[...]).astype(BF16)
    grad, term = norm_back(upstream[i].astype(F32), branch, scale, gain[...])
    return grad.astype(BF16), (term,)


@with_sums(2)
def body_back(i, delta, ins, outs):
    hidden, branch, upstream, gain_attn, gain_ffn = ins
    hid, y1 = hidden[i], branch[i]
    part, term_ffn = norm_back(delta, hid, inverse_rms(hid), gain_ffn[...])
    hid_grad = upstream[i].astype(F32) + part
    outs[0][i] = hid_grad
    grad, term_attn = norm_back(hid_grad, y1, inverse_rms(y1), gain_attn[...])
    return grad.astype(BF16), (term_ffn, term_attn)


@with_sums(1)
def body_last(i, delta, ins, outs):
    tokens, hidden_grad, gain = ins
    values = tokens[i].astype(F32)
    part, term = norm_back(delta, values, inverse_rms(values), gain[...])
    return (hidden_grad[i] + part).astype(BF16), (term,)


def scores(q, k):
    s = jnp.einsum("bqd,bkd->bqk", q, k, preferred_element_type=F32) * QUERY_FACTOR
    t = jnp.tanh(s / SOFT_CAP)
    length = q.shape[1]
    allowed = jnp.arange(length)[None, :] <= jnp.arange(length)[:, None]
    return t, jnp.where(allowed[None], SOFT_CAP * t, MASKED)


def attend(q, k, v):
    _, c = scores(q, k)
    top = jnp.max(c, axis=-1, keepdims=True)
    lse = top + jnp.log(jnp.sum(jnp.exp(c - top), axis=-1, keepdims=True))
    p = jnp.exp(c - lse).astype(BF16)
    return jnp.einsum("bqk,bkd->bqd", p, v, preferred_element_type=F32).astype(BF16), lse


def attend_back(q, k, v, o, do, lse):
    t, c = scores(q, k)
    p = jnp.exp(c - lse)
    dd = jnp.sum(do.astype(F32) * o.astype(F32), axis=-1, keepdims=True)
    dp = jnp.einsum("bqd,bkd->bqk", do, v, preferred_element_type=F32)
    ds = (p * (dp - dd) * (1.0 - t * t) * QUERY_FACTOR).astype(BF16)
    dv = jnp.einsum("bqk,bqd->bkd", p.astype(BF16), do, preferred_element_type=F32)
    dk = jnp.einsum("bqk,bqd->bkd", ds, q, preferred_element_type=F32)
    dq = jnp.einsum("bqk,bkd->bqd", ds, k, preferred_element_type=F32)
    return dq.astype(BF16), dk.astype(BF16), dv.astype(BF16)


def dot_f32(a, b):
    return jnp.dot(a, b, preferred_element_type=F32)


def dot_nt(a, b):
    return lax.dot_general(a, b, (((1,), (1,)), ((), ())), preferred_element_type=F32)


def dot_tn(a, b):
    return lax.dot_general(a, b, (((0,), (0,)), ((), ())), preferred_element_type=F32)


def swap(x, axis):
    return lax.all_to_all(x, axis, split_axis=0, concat_axis=0, tiled=True)


def on_device_plane(
    ns, nf,
    tokens, pre_attn_gain, qkv_weight, out_weight, post_attn_gain, pre_ffn_gain,
    gate_up_weight, down_weight, post_ffn_gain, out_grad,
):
    _, chunk, width = tokens.shape
    length = chunk * ns
    spp = nf // ns
    r = chunk // nf
    rows = spp * ns
    group = H // KV
    ff = down_weight.shape[0]
    ffp = -(-ff // LANES) * LANES
    depth = qkv_weight.shape[0]

    q_cols = qkv_weight[:, : H * HD].reshape(depth, H, HD)
    k_cols = jnp.repeat(qkv_weight[:, H * HD : (H + KV) * HD].reshape(depth, KV, HD), group, axis=1)
    v_cols = jnp.repeat(qkv_weight[:, (H + KV) * HD :].reshape(depth, KV, HD), group, axis=1)
    w_qkv = jnp.concatenate([q_cols, k_cols, v_cols], axis=2).transpose(1, 0, 2)
    w_qkv = swap(w_qkv, "fsdp").reshape(nf * depth, 3 * HD)
    w_gu = swap(split_columns(gate_up_weight, nf, ff, ffp), "fsdp")
    w_gu = w_gu.reshape(nf * depth, 2 * ffp)
    w_down = jnp.pad(down_weight, ((0, ffp - ff), (0, 0)))

    gains = [g.reshape(1, width) for g in (pre_attn_gain, post_attn_gain, pre_ffn_gain, post_ffn_gain)]
    flat = (rows * nf * r, width)
    shape = (rows, nf, r, width)

    a_full, x_own, g_own = enter(
        nf, ns, tokens.reshape(nf, r, width), out_grad.reshape(nf, r, width), gains[0]
    )
    x_own, g_own = x_own.reshape(rows, r, width), g_own.reshape(rows, r, width)
    a_full = a_full.reshape(flat)
    qkv = dot_f32(a_full, w_qkv).astype(BF16)
    q, k, v = (qkv[:, i * HD : (i + 1) * HD].reshape(spp, length, HD) for i in range(3))
    o, lse = attend(q, k, v)
    o_flat = o.reshape(-1, HD)
    y1_terms = dot_f32(o_flat, out_weight).astype(BF16).reshape(shape)
    n_full, y1, hidden = middle(
        "mid", 2, nf, ns, body_mid, y1_terms, [x_own, gains[1], gains[2]], [F32, F32]
    )
    n_full = n_full.reshape(flat)
    gu = dot_f32(n_full, w_gu)
    gate, up = gu[:, :ffp], gu[:, ffp:]
    activated, derivative = gelu_pair(gate)
    mixed = (activated * up).astype(BF16)
    y2_terms = dot_f32(mixed, w_down).astype(BF16).reshape(shape)
    dy2_full, out_own, post_ffn_term = middle(
        "turn", 3, nf, ns, body_turn, y2_terms, [hidden, g_own, gains[3]], [BF16]
    )
    dy2_full = dy2_full.reshape(flat)
    down_wg = dot_tn(mixed, dy2_full)[:ff].astype(BF16)
    dm = dot_nt(dy2_full, w_down)
    dgu = jnp.concatenate([dm * up * derivative, dm * activated], axis=1).astype(BF16)
    dn_terms = dot_nt(dgu, w_gu).astype(BF16).reshape(shape)
    gu_wg = dot_tn(n_full, dgu).astype(BF16).reshape(nf, depth, 2 * ffp)
    pieces = next(n for n in (9, 6, 3, 2, 1) if ff % (16 * n) == 0)
    dy1_full, hidden_grad, pre_ffn_term, post_attn_term, down_wg = middle(
        "back", 4, nf, ns, body_back, dn_terms, [hidden, y1, g_own, gains[1], gains[2]], [F32],
        down_wg.reshape(pieces, ff // pieces, width), (0, 0, 1, 2, 4, 4, 2, 2, 2),
    )
    dy1_full = dy1_full.reshape(flat)
    do = dot_nt(dy1_full, out_weight).astype(BF16).reshape(o.shape)
    out_wg = dot_tn(o_flat, dy1_full).astype(BF16)
    dq, dk, dv = attend_back(q, k, v, o, do, lse)
    dqkv = jnp.concatenate([dq, dk, dv], axis=2).reshape(-1, 3 * HD)
    da_terms = dot_nt(dqkv, w_qkv).astype(BF16).reshape(shape)
    qkv_wg = dot_tn(a_full, dqkv).astype(BF16).reshape(nf, depth, 3 * HD)
    terms = jnp.concatenate(
        [jnp.zeros((1, width), F32), post_attn_term, pre_ffn_term, post_ffn_term, jnp.zeros((4, width), F32)]
    )
    layer_out, tokens_grad, gain_sums, gu_wg, qkv_wg, out_wg = leave(
        nf, ns, body_last, da_terms, x_own, hidden_grad, gains[0],
        out_own.reshape(spp, ns, r, width), terms, gu_wg, qkv_wg, out_wg.reshape(2, HD // 2, width),
    )
    gu_wg, qkv_wg = join_columns(gu_wg, qkv_wg, nf, ff)
    return (
        layer_out.reshape(1, chunk, width),
        tokens_grad.astype(F32).reshape(1, chunk, width),
        gain_sums[0],
        qkv_wg,
        out_wg.reshape(HD, width).astype(F32),
        gain_sums[1],
        gain_sums[2],
        gu_wg,
        down_wg.reshape(ff, width).astype(F32),
        gain_sums[3],
    )


def gathered_norm_back(upstream, values, inv_scale, gains):
    weighted = upstream * gains
    inner_mean = jnp.mean(weighted * values, axis=-1, keepdims=True)
    gradient = inv_scale * weighted - values * (inv_scale * inv_scale * inv_scale) * inner_mean
    gain_grad = jnp.sum(upstream * values * inv_scale, axis=0)
    return (gradient, gain_grad)


def batched_contraction(pattern, left_side, right_side):
    return jnp.einsum(pattern, left_side, right_side, preferred_element_type=jnp.float32)


def gathered_capped_scores(block_of_queries, key_row_slices, offset):
    amount = block_of_queries.shape[0]
    key_count = key_row_slices.shape[0]
    unscaled_logits = (
        batched_contraction("olv,ilv->loi", block_of_queries, key_row_slices) * QUERY_FACTOR
    )
    tanh_part = jnp.tanh(unscaled_logits / SOFT_CAP)
    allowed = (
        jnp.arange(key_count, dtype=jnp.int32)[None, :]
        <= (offset + jnp.arange(amount, dtype=jnp.int32))[:, None]
    )
    capped = jnp.where(allowed[None], SOFT_CAP * tanh_part, MASKED)
    return (tanh_part, capped)


def gathered_attend(queries, key_row_slices, value_row_slices):
    length = queries.shape[0]
    block_size = min(512, length)
    blocks = length // block_size

    def one_block(block_id):
        offset = block_id * block_size
        block_of_queries = lax.dynamic_slice_in_dim(queries, offset, block_size, 0)
        tanh_part, capped = gathered_capped_scores(block_of_queries, key_row_slices, offset)
        biggest = jnp.max(capped, axis=-1, keepdims=True)
        logsum = biggest + jnp.log(jnp.sum(jnp.exp(capped - biggest), axis=-1, keepdims=True))
        attention_probabilities = jnp.exp(capped - logsum).astype(jnp.bfloat16)
        layer_result = batched_contraction(
            "vxn,nvs->xvs", attention_probabilities, value_row_slices
        ).astype(jnp.bfloat16)
        return (layer_result, logsum[..., 0])

    outputs, logsums = lax.map(one_block, jnp.arange(blocks, dtype=jnp.int32))
    return (outputs.reshape(queries.shape), logsums)


def gathered_attend_back(queries, key_row_slices, value_row_slices, outputs, out_delta, logsums):
    length = queries.shape[0]
    block_size = min(512, length)
    blocks = length // block_size
    row_dots = batched_contraction("qbd,qbd->bq", out_delta, outputs)

    def one_block(carried, inputs):
        key_accumulator, value_accumulator = carried
        block_id, block_logsum = inputs
        offset = block_id * block_size
        block_of_queries = lax.dynamic_slice_in_dim(queries, offset, block_size, 0)
        block_correction = lax.dynamic_slice_in_dim(out_delta, offset, block_size, 0)
        tanh_part, capped = gathered_capped_scores(block_of_queries, key_row_slices, offset)
        attention_probabilities = jnp.exp(capped - block_logsum[..., None])
        probability_gradients = batched_contraction(
            "olv,ilv->loi", block_correction, value_row_slices
        )
        dots_block = lax.dynamic_slice_in_dim(row_dots, offset, block_size, 1)
        logit_gradients = (
            attention_probabilities
            * (probability_gradients - dots_block[..., None])
            * (1.0 - tanh_part * tanh_part)
            * QUERY_FACTOR
        ).astype(jnp.bfloat16)
        rounded_values = attention_probabilities.astype(jnp.bfloat16)
        value_accumulator = value_accumulator + batched_contraction(
            "pfm,fpg->mpg", rounded_values, block_correction
        )
        key_accumulator = key_accumulator + batched_contraction(
            "pfm,fpg->mpg", logit_gradients, block_of_queries
        )
        query_gradient = batched_contraction(
            "vxn,nvs->xvs", logit_gradients, key_row_slices
        ).astype(jnp.bfloat16)
        return ((key_accumulator, value_accumulator), query_gradient)

    zero_acc = jnp.zeros(key_row_slices.shape, jnp.float32)
    (key_accumulator, value_accumulator), query_grads = lax.scan(
        one_block, (zero_acc, zero_acc), (jnp.arange(blocks, dtype=jnp.int32), logsums)
    )
    return (
        query_grads.reshape(queries.shape),
        key_accumulator.astype(jnp.bfloat16),
        value_accumulator.astype(jnp.bfloat16),
    )


def gathered_project(activations, weight_shard):
    return jnp.dot(
        activations,
        lax.all_gather(weight_shard, "fsdp", axis=0, tiled=True),
        preferred_element_type=jnp.float32,
    )


def gathered_project_back(gradient, weight_shard):
    return lax.dot_general(
        gradient,
        lax.all_gather(weight_shard, "fsdp", axis=0, tiled=True),
        (((1,), (1,)), ((), ())),
        preferred_element_type=jnp.float32,
    )


def term_maker(activations, gradient):
    return lax.dot_general(
        activations, gradient, (((0,), (0,)), ((), ())), preferred_element_type=jnp.float32
    )


def weight_term(activations, gradient):
    sliced = lax.psum_scatter(
        term_maker(activations, gradient).astype(jnp.bfloat16),
        "fsdp",
        scatter_dimension=0,
        tiled=True,
    )
    return lax.psum(sliced, "seq").astype(jnp.float32)


def gathered_on_device(
    tokens,
    pre_attn_gain,
    qkv_weight,
    out_weight,
    post_attn_gain,
    pre_ffn_gain,
    gate_up_weight,
    down_weight,
    post_ffn_gain,
    out_grad,
):
    groups, local_len, width = tokens.shape
    row_count = groups * local_len
    head_repeat = H // KV
    ff = gate_up_weight.shape[1] // 2
    residual_in = tokens.reshape(row_count, width).astype(jnp.float32)
    scale_one = inverse_rms(residual_in)
    normed_in = (residual_in * scale_one * pre_attn_gain).astype(jnp.bfloat16)
    projected = gathered_project(normed_in, qkv_weight).astype(jnp.bfloat16)
    queries = projected[:, : H * HD].reshape(groups, local_len, H, HD)
    key_row_slices = jnp.repeat(
        projected[:, H * HD : (H + KV) * HD].reshape(groups, local_len, KV, HD), head_repeat, axis=2
    )
    value_row_slices = jnp.repeat(
        projected[:, (H + KV) * HD :].reshape(groups, local_len, KV, HD), head_repeat, axis=2
    )
    head_queries, head_keys, head_values = (
        lax.all_to_all(queries, "seq", split_axis=2, concat_axis=1, tiled=True),
        lax.all_to_all(key_row_slices, "seq", split_axis=2, concat_axis=1, tiled=True),
        lax.all_to_all(value_row_slices, "seq", split_axis=2, concat_axis=1, tiled=True),
    )
    head_out, logsums = jax.vmap(gathered_attend)(head_queries, head_keys, head_values)
    attn_out = lax.all_to_all(head_out, "seq", split_axis=1, concat_axis=2, tiled=True).reshape(
        row_count, H * HD
    )
    branch_one = gathered_project(attn_out, out_weight)
    scale_two = inverse_rms(branch_one)
    hidden = residual_in + branch_one * scale_two * post_attn_gain
    scale_three = inverse_rms(hidden)
    normed_mid = (hidden * scale_three * pre_ffn_gain).astype(jnp.bfloat16)
    gate_up = gathered_project(normed_mid, gate_up_weight)
    gate_part = gate_up[:, :ff]
    up_part = gate_up[:, ff:]
    activated, derivative = gelu_pair(gate_part)
    mixed = (activated * up_part).astype(jnp.bfloat16)
    branch_two = gathered_project(mixed, down_weight)
    scale_four = inverse_rms(branch_two)
    layer_out = (
        (hidden + branch_two * scale_four * post_ffn_gain)
        .astype(jnp.bfloat16)
        .reshape(groups, local_len, width)
    )
    upstream = out_grad.reshape(row_count, width).astype(jnp.float32)
    branch_two_grad, post_ffn_term = gathered_norm_back(upstream, branch_two, scale_four, post_ffn_gain)
    branch_two_grad = branch_two_grad.astype(jnp.bfloat16)
    down_wgrad = weight_term(mixed, branch_two_grad)
    mixed_grad = gathered_project_back(branch_two_grad, down_weight)
    gate_up_grad = jnp.concatenate(
        [mixed_grad * up_part * derivative, mixed_grad * activated], axis=1
    ).astype(jnp.bfloat16)
    gate_up_wgrad = weight_term(normed_mid, gate_up_grad)
    normed_mid_grad = gathered_project_back(gate_up_grad, gate_up_weight)
    hidden_part, pre_ffn_term = gathered_norm_back(normed_mid_grad, hidden, scale_three, pre_ffn_gain)
    hidden_grad = upstream + hidden_part
    branch_one_grad, post_attn_term = gathered_norm_back(hidden_grad, branch_one, scale_two, post_attn_gain)
    branch_one_grad = branch_one_grad.astype(jnp.bfloat16)
    out_wgrad = weight_term(attn_out, branch_one_grad)
    attn_grad = (
        gathered_project_back(branch_one_grad, out_weight)
        .astype(jnp.bfloat16)
        .reshape(groups, local_len, H, HD)
    )
    head_delta = lax.all_to_all(attn_grad, "seq", split_axis=2, concat_axis=1, tiled=True)
    query_gradient, key_grad, value_grad = jax.vmap(gathered_attend_back)(
        head_queries, head_keys, head_values, head_out, head_delta, logsums
    )
    query_tok, key_tok, value_tok = (
        lax.all_to_all(query_gradient, "seq", split_axis=1, concat_axis=2, tiled=True),
        lax.all_to_all(key_grad, "seq", split_axis=1, concat_axis=2, tiled=True),
        lax.all_to_all(value_grad, "seq", split_axis=1, concat_axis=2, tiled=True),
    )
    key_sum = (
        key_tok.astype(jnp.float32)
        .reshape(groups, local_len, KV, head_repeat, HD)
        .sum(axis=3)
        .astype(jnp.bfloat16)
    )
    value_sum = (
        value_tok.astype(jnp.float32)
        .reshape(groups, local_len, KV, head_repeat, HD)
        .sum(axis=3)
        .astype(jnp.bfloat16)
    )
    qkv_grad = jnp.concatenate(
        [
            query_tok.reshape(row_count, H * HD),
            key_sum.reshape(row_count, KV * HD),
            value_sum.reshape(row_count, KV * HD),
        ],
        axis=1,
    )
    qkv_wgrad = weight_term(normed_in, qkv_grad)
    normed_in_grad = gathered_project_back(qkv_grad, qkv_weight)
    input_part, pre_attn_term = gathered_norm_back(normed_in_grad, residual_in, scale_one, pre_attn_gain)
    tokens_grad = (hidden_grad + input_part).reshape(groups, local_len, width)
    gain_sums = lax.psum(
        (pre_attn_term, post_attn_term, pre_ffn_term, post_ffn_term), ("seq", "fsdp")
    )
    return (
        layer_out,
        tokens_grad,
        gain_sums[0],
        qkv_wgrad,
        out_wgrad,
        gain_sums[1],
        gain_sums[2],
        gate_up_wgrad,
        down_wgrad,
        gain_sums[3],
    )


def solution(mesh):
    ns, nf = mesh.shape["seq"], mesh.shape["fsdp"]
    token_spec, row_spec = P("fsdp", "seq", None), P("fsdp", None)
    in_specs = (
        token_spec, P(), row_spec, row_spec, P(), P(), row_spec, row_spec, P(), token_spec,
    )
    out_specs = (
        token_spec, token_spec, P(), row_spec, row_spec, P(), P(), row_spec, row_spec, P(),
    )

    def on_device(*args):
        if nf == 8 and nf == H and nf % ns == 0 and ns == 4 and args[0].shape[0] == 1:
            return on_device_plane(ns, nf, *args)
        return gathered_on_device(*args)

    return jax.shard_map(
        on_device, mesh=mesh, in_specs=in_specs, out_specs=out_specs, check_vma=False
    )
```

```python
import functools
import math

import jax
import jax.numpy as jnp
from jax import lax
from jax.experimental import pallas as pl
from jax.experimental.pallas import tpu as pltpu
from jax.sharding import PartitionSpec as P

H = 8
KV = 4
HD = 256

EPSILON = 1e-06
SOFT_CAP = 50.0
QUERY_FACTOR = 0.0625
GELU_COEFF = math.sqrt(2.0 / math.pi)
CUBIC = 0.044715
MASKED = -1e30
MESH = pl.DeviceIdType.MESH
F32 = jnp.float32
BF16 = jnp.bfloat16
LANES = 128


def inverse_rms(values):
    return lax.rsqrt(jnp.mean(values * values, axis=-1, keepdims=True) + EPSILON)


def norm_back(upstream, values, inv_scale, gains):
    weighted = upstream * gains
    inner_mean = jnp.mean(weighted * values, axis=-1, keepdims=True)
    gradient = inv_scale * weighted - values * (inv_scale * inv_scale * inv_scale) * inner_mean
    gain_grad = jnp.sum(upstream * values * inv_scale, axis=0, keepdims=True)
    return (gradient, gain_grad)


def gelu_pair(values):
    inner_part = GELU_COEFF * (values + CUBIC * values * values * values)
    tanh_part = jnp.tanh(inner_part)
    activated = 0.5 * values * (1.0 + tanh_part)
    derivative = 0.5 * (1.0 + tanh_part) + 0.5 * values * (
        1.0 - tanh_part * tanh_part
    ) * GELU_COEFF * (1.0 + 3.0 * CUBIC * values * values)
    return (activated, derivative)


class Place:
    def __init__(self, nf, ns):
        self.nf, self.ns = nf, ns
        self.me, self.z = lax.axis_index("fsdp"), lax.axis_index("seq")
        core, xpos, ypos = self.me % 2, (self.me // 2) % 2, self.me // 4
        self.step = 1 - 2 * core
        self.mate = self.me + self.step
        self.xn = self.me + 2 - 4 * xpos
        self.yn = self.me + 4 - 8 * ypos
        self.diag = self.xn + 4 - 8 * ypos

    def plane_peers(self):
        return [(self.me + d) % self.nf for d in range(1, self.nf)]

    def line_peers(self):
        return [(self.z + d) % self.ns for d in range(1, self.ns)]

    def greet(self, near, plane, line):
        barrier = pltpu.get_barrier_semaphore()
        to = [{"fsdp": p} for p in (self.plane_peers() if plane else (self.mate, self.xn, self.yn) if near else ())]
        to += [{"seq": p} for p in (self.line_peers() if line else ())]
        for device in to:
            pl.semaphore_signal(barrier, inc=1, device_id=device, device_id_type=MESH)
        pl.semaphore_wait(barrier, len(to))


class Wire:
    def __init__(self, lsem, ssem, rsem):
        self.lsem, self.ssem, self.rsem = lsem, ssem, rsem
        self.sent, self.kept = [], []

    def send(self, src, dst, device):
        k = len(self.sent)
        copy = pltpu.make_async_remote_copy(
            src_ref=src, dst_ref=dst, send_sem=self.ssem.at[k], recv_sem=self.rsem.at[k],
            device_id=device, device_id_type=MESH,
        )
        copy.start()
        self.sent.append(copy)
        return copy

    def near(self, src, dst, to):
        return self.send(src, dst, {"fsdp": to})

    def keep(self, src, dst):
        copy = pltpu.make_async_copy(src, dst, self.lsem.at[len(self.kept)])
        copy.start()
        self.kept.append(copy)
        return copy

    def flush(self):
        for copy in self.sent:
            copy.wait_send()


def each(count, f):
    def one(i, _):
        f(i)
        return 0

    lax.fori_loop(0, count, one, 0)


def halves_of(rows):
    return pl.ds(0, rows // 2), pl.ds(rows // 2, rows // 2)


def reduce_start(at, wire, part, acc, other):
    order = (at.diag, at.xn, at.yn, at.me)
    return [wire.keep(part.at[:, b], acc.at[k]) for k, b in enumerate(order)]


def reduce_in_plane(at, wire, own, part, acc, other, ra, rb, rx, ry):
    rows = acc.shape[1]
    half = rows // 2
    h0, h1 = halves_of(rows)
    order = (at.diag, at.xn, at.yn, at.me)
    mates = [wire.near(part.at[:, b + at.step], other.at[k], at.mate) for k, b in enumerate(order)]
    yield

    def add(dst, src, lo, count):
        def one(i):
            dst[lo + i] = (dst[lo + i].astype(F32) + src[i].astype(F32)).astype(BF16)

        each(count, one)

    def join(k):
        own[k].wait()
        mates[k].wait_recv()
        add(acc.at[k], other.at[k], 0, rows)

    join(0)
    ca = wire.near(acc.at[0, h0], ra, at.yn)
    cb = wire.near(acc.at[0, h1], rb, at.xn)
    yield
    join(1)
    cx1 = wire.near(acc.at[1, h1], rx.at[h1], at.xn)
    join(2)
    cy0 = wire.near(acc.at[2, h0], ry.at[h0], at.yn)
    yield
    ca.wait_recv()
    add(acc.at[1], ra, 0, half)
    cx0 = wire.near(acc.at[1, h0], rx.at[h0], at.xn)
    cb.wait_recv()
    add(acc.at[2], rb, half, half)
    cy1 = wire.near(acc.at[2, h1], ry.at[h1], at.yn)
    own[3].wait()
    mates[3].wait_recv()
    yield
    cx1.wait_recv()
    cy0.wait_recv()
    yield
    cx0.wait_recv()
    cy1.wait_recv()


def gather_in_plane(at, wire, block, full):
    h0, h1 = halves_of(block.shape[0])
    me, xn, yn, diag, mate = at.me, at.xn, at.yn, at.diag, at.mate
    keep = wire.keep(block, full.at[:, me])

    def pass_on(copy, where, blk, to):
        copy.wait_recv()
        return wire.near(full.at[where, blk], full.at[where, blk], to)

    y0 = wire.near(block.at[h0], full.at[h0, me], yn)
    x1 = wire.near(block.at[h1], full.at[h1, me], xn)
    y1 = wire.near(block.at[h1], full.at[h1, me], yn)
    x0 = wire.near(block.at[h0], full.at[h0, me], xn)
    last = [wire.near(block, full.at[:, me], mate)]
    yield
    gx = pass_on(y0, h0, yn, xn)
    last.append(wire.near(full.at[h0, yn], full.at[h0, yn], mate))
    gy = pass_on(x1, h1, xn, yn)
    last.append(wire.near(full.at[h1, xn], full.at[h1, xn], mate))
    yield
    last.append(pass_on(y1, h1, yn, mate))
    last.append(pass_on(x0, h0, xn, mate))
    yield
    last.append(pass_on(gx, h0, diag, mate))
    last.append(pass_on(gy, h1, diag, mate))
    yield
    for copy in last:
        copy.wait_recv()
    keep.wait()


def weave(main, others=(), counts=()):
    others, counts = list(others), list(counts)
    for _ in main:
        for _ in range(counts.pop(0) if counts else 0):
            if others:
                others.pop(0)()
    for other in others:
        other()


class LineSum:
    def __init__(self, at, items, sems):
        self.z, self.items, self.sems = at.z, items, sems
        self.outer = at.z % 3 == 0
        self.inner = at.z % 3 != 0
        self.pair = at.z + 1 - 2 * (at.z % 2)
        self.across = 3 - at.z

    def copy(self, stage, k):
        own, in1, in2, out = self.items[k]
        src, dst, to = ((own, in1, self.pair), (in1, in2, self.across), (in2, out, self.pair))[stage]
        send, recv = self.sems[2 * stage], self.sems[2 * stage + 1]
        return pltpu.make_async_remote_copy(
            src_ref=src, dst_ref=dst, send_sem=send.at[k], recv_sem=recv.at[k],
            device_id={"seq": to}, device_id_type=MESH,
        )

    def kept(self, k):
        return pltpu.make_async_copy(self.items[k][2], self.items[k][3], self.sems[6].at[k])

    @staticmethod
    def add(dst, src):
        def one(i):
            where = pl.ds(pl.multiple_of(i * 16, 16), 16)
            dst[where] = (dst[where].astype(F32) + src[where].astype(F32)).astype(BF16)

        each(dst.shape[0] // 16, one)

    def launch(self, k):
        @pl.when(self.outer)
        def _():
            self.copy(0, k).start()

    def first(self, k):
        @pl.when(self.inner)
        def _():
            self.copy(0, k).wait_recv()
            self.add(self.items[k][1], self.items[k][0])
            self.copy(1, k).start()

    def second(self, k):
        @pl.when(self.inner)
        def _():
            self.copy(1, k).wait_recv()
            self.add(self.items[k][2], self.items[k][1])
            self.copy(2, k).start()
            self.kept(k).start()

    def steps(self):
        n = len(self.items)
        out = []
        for k in range(n + 1):
            if k < n:
                out.append(functools.partial(self.first, k))
            if k > 0:
                out.append(functools.partial(self.second, k - 1))
        return out

    def end_one(self, k, seen=False):
        @pl.when(self.outer)
        def _():
            self.copy(0, k).wait_send()
            if not seen:
                self.copy(2, k).wait_recv()

        @pl.when(self.inner)
        def _():
            self.copy(1, k).wait_send()
            self.copy(2, k).wait_send()
            if not seen:
                self.kept(k).wait()

    def end(self):
        for k in range(len(self.items)):
            self.end_one(k)

    @staticmethod
    def semaphores(n):
        return [pltpu.SemaphoreType.DMA((n,))] * 7


def enter_kernel(nf, ns, ff, *refs):
    tok, grad, gain, wqkv, wgu = refs[:5]
    full, x_own, g_own, heads, sorted_out = refs[5:10]
    xs, gs, xo, go, block, wide, sorted_, lsem, ssem, rsem = refs[10:]
    at, wire = Place(nf, ns), Wire(lsem, ssem, rsem)
    spp = nf // ns
    group = H // KV
    keeps = [wire.keep(tok.at[at.me], xs.at[at.me]), wire.keep(grad.at[at.me], gs.at[at.me])]
    load = wire.keep(wgu, wide)

    def columns(p):
        starts = (p * HD, H * HD + (p // group) * HD, (H + KV) * HD + (p // group) * HD)
        return [
            (wqkv.at[:, pl.ds(pl.multiple_of(lo, HD), HD)], heads.at[at.me, :, pl.ds(k * HD, HD)])
            for k, lo in enumerate(starts)
        ]

    own_heads = [wire.keep(*pair) for pair in columns(at.me)]
    at.greet(True, True, True)
    first = [
        [wire.near(src.at[p], dst.at[at.me], p) for p in at.plane_peers()]
        for src, dst in ((tok, xs), (grad, gs))
    ]
    head_moves = [wire.near(*pair, p) for p in at.plane_peers() for pair in columns(p)]
    second, own = [], []

    def stage(k, src, dst):
        keeps[k].wait()
        for copy in first[k]:
            copy.wait_recv()
        second.append(
            [
                wire.send(src.at[pl.ds(p * spp, spp)], dst.at[:, at.z], {"seq": p})
                for p in at.line_peers()
            ]
        )
        own.append(wire.keep(src.at[pl.ds(at.z * spp, spp)], dst.at[:, at.z]))

    stage(0, xs, xo)
    stage(1, gs, go)
    load.wait()
    ffp = sorted_.shape[2] // 2

    def sort(i):
        where = pl.ds(pl.multiple_of(i * 16, 16), 16)
        for f in range(nf):
            for g in range(2):
                piece = wide[where, (g * nf + f) * ff : (g * nf + f + 1) * ff]
                if ffp > ff:
                    piece = jnp.concatenate([piece, jnp.zeros((16, ffp - ff), BF16)], axis=1)
                sorted_[f, where, g * ffp : (g + 1) * ffp] = piece

    each(wide.shape[0] // 16, sort)
    outs = [wire.keep(sorted_, sorted_out)]
    own[0].wait()
    for copy in second[0]:
        copy.wait_recv()
    outs.append(wire.keep(xo, x_own))

    def one(i):
        values = xo[i // ns, i % ns].astype(F32)
        block[i] = (values * inverse_rms(values) * gain[...]).astype(BF16)

    each(nf, one)
    weave(gather_in_plane(at, wire, block, full))
    own[1].wait()
    for copy in second[1] + head_moves:
        copy.wait_recv()
    outs.append(wire.keep(go, g_own))
    for copy in outs + own_heads:
        copy.wait()
    wire.flush()


def enter(nf, ns, tokens, grads, gain, wqkv, wgu, ffp):
    _, r, width = tokens.shape
    spp = nf // ns
    depth = wqkv.shape[0]
    own = jax.ShapeDtypeStruct((spp, ns, r, width), BF16)
    anys = pl.BlockSpec(memory_space=pl.ANY)
    n_send = 2 * (nf - 1) + 2 * (ns - 1) + 13 + 3 * (nf - 1)
    return pl.pallas_call(
        functools.partial(enter_kernel, nf, ns, wgu.shape[1] // (2 * nf)),
        name="enter",
        out_shape=[jax.ShapeDtypeStruct((nf, nf, r, width), BF16), own, own]
        + [jax.ShapeDtypeStruct((nf, depth, c), BF16) for c in (3 * HD, 2 * ffp)],
        in_specs=[anys, anys, pl.BlockSpec(memory_space=pltpu.VMEM), anys, anys],
        out_specs=[anys] * 5,
        scratch_shapes=[pltpu.VMEM((nf, r, width), BF16)] * 2
        + [pltpu.VMEM((spp, ns, r, width), BF16)] * 2
        + [pltpu.VMEM((nf, r, width), BF16)]
        + [pltpu.VMEM(wgu.shape, BF16), pltpu.VMEM((nf, depth, 2 * ffp), BF16)]
        + [pltpu.SemaphoreType.DMA((12,))]
        + [pltpu.SemaphoreType.DMA((n_send,))] * 2,
        compiler_params=pltpu.CompilerParams(collective_id=1, has_side_effects=True),
    )(tokens, grads, gain, wqkv, wgu)


def go_home(at, wire, src, buf, out):
    spp = at.nf // at.ns
    own, line = [], []
    for s in range(spp):
        own.append(wire.keep(src.at[s * at.ns + at.z], buf.at[at.z * spp + s]))
        line += [
            wire.send(src.at[s * at.ns + p], buf.at[at.z * spp + s], {"seq": p})
            for p in at.line_peers()
        ]
    yield
    for copy in own:
        copy.wait()
    for copy in line:
        copy.wait_recv()
    home = wire.keep(buf.at[at.me], out.at[at.me])
    away = [wire.near(buf.at[p], out.at[at.me], p) for p in at.plane_peers()]
    yield
    home.wait()
    for copy in away:
        copy.wait_recv()


def middle_kernel(nf, ns, n_in, n_own, body, homing, plan, *refs):
    refs = list(refs)
    part, ins = refs[0], refs[1 : 1 + n_in]
    del refs[: 1 + n_in]
    grad = refs.pop(0) if plan else None
    full = refs.pop(0)
    outs = [refs.pop(0) for _ in range(n_own)]
    summed = refs.pop(0) if plan else None
    acc, other, ra, rb, rx, ry, block, lsem, ssem, rsem = refs[:10]
    del refs[:10]
    at, wire = Place(nf, ns), Wire(lsem, ssem, rsem)
    own = reduce_start(at, wire, part, acc, other)
    at.greet(True, homing, plan or homing)
    line = None
    if homing:
        home, outs[0], buf = outs[0], refs[0], refs[1]
    if plan:
        in1, in2 = refs[:2]
        line = LineSum(at, [(grad.at[k], in1.at[k], in2.at[k], summed.at[k]) for k in range(grad.shape[0])], refs[2:])

    def main():
        yield from reduce_in_plane(at, wire, own, part, acc, other, ra, rb, rx, ry)
        work_on_sum(body, acc, other, rx, ry, ins, outs, block)
        going = go_home(at, wire, outs[0], buf, home) if homing else iter(())
        next(going, None)
        yield from gather_in_plane(at, wire, block, full)
        for _ in going:
            pass

    if plan:
        for k in range(len(line.items)):
            line.launch(k)
        weave(main(), line.steps(), plan)
        line.end()
    else:
        weave(main())
    wire.flush()


def work_on_sum(body, acc, other, rx, ry, ins, outs, block):
    def one(i, sums):
        total = (acc[3, i].astype(F32) + other[3, i].astype(F32)) + (
            rx[i].astype(F32) + ry[i].astype(F32)
        )
        block[i], extra = body(i, total, ins, outs)
        return tuple(s + e for s, e in zip(sums, extra))

    rows, _, width = block.shape
    zero = tuple(jnp.zeros((1, width), F32) for _ in range(body.n_sums))
    sums = lax.fori_loop(0, rows, one, zero)
    for s, ref in zip(sums, outs[len(outs) - body.n_sums :]):
        ref[...] = s


def sum_scratch(rows, r, width):
    shape, half = (rows, r, width), (rows // 2, r, width)
    return [pltpu.VMEM((4,) + shape, BF16)] * 2 + [pltpu.VMEM(half, BF16)] * 2 + [pltpu.VMEM(shape, BF16)] * 3


def middle(name, cid, nf, ns, body, part, ins, own_types, homing=False, grad=None, plan=None):
    rows, _, r, width = part.shape
    vmem, anys = pl.BlockSpec(memory_space=pltpu.VMEM), pl.BlockSpec(memory_space=pl.ANY)
    out_shape = [jax.ShapeDtypeStruct(part.shape, BF16)]
    out_shape += [jax.ShapeDtypeStruct((rows, r, width), t) for t in own_types]
    out_shape += [jax.ShapeDtypeStruct((1, width), F32)] * body.n_sums
    n_own = len(out_shape) - 1
    in_specs, out_specs = [anys] + [vmem] * len(ins), [anys] + [vmem] * n_own
    n_send = 23 + ((ns - 1) * (nf // ns) + nf - 1 if homing else 0)
    scratch = sum_scratch(rows, r, width)
    scratch += [pltpu.SemaphoreType.DMA((8,))] + [pltpu.SemaphoreType.DMA((n_send,))] * 2
    operands = [part, *ins]
    if homing:
        out_specs[1] = anys
        scratch += [pltpu.VMEM((nf, r, width), own_types[0])] * 2
    if plan:
        operands.append(grad)
        in_specs.append(vmem)
        out_shape.append(jax.ShapeDtypeStruct(grad.shape, BF16))
        out_specs.append(anys)
        scratch += [pltpu.VMEM(grad.shape, BF16)] * 2 + LineSum.semaphores(grad.shape[0])
    return pl.pallas_call(
        functools.partial(middle_kernel, nf, ns, len(ins), n_own, body, homing, plan),
        name=name,
        out_shape=out_shape,
        in_specs=in_specs,
        out_specs=out_specs,
        scratch_shapes=scratch,
        compiler_params=pltpu.CompilerParams(collective_id=cid, has_side_effects=True),
    )(*operands)


def leave_kernel(nf, ns, body, rest, *refs):
    part, tokens, hid_grad, gain, terms, done, todo, qkv, wout = refs[:9]
    tok_out, gain_out, rows_out, qkv_out, wout_out = refs[9:14]
    (acc, other, ra, rb, rx, ry, block, bz, gl, gt, gp, gz, held, up_own, up1, up2, up_sum,
     qkv_in, qkv_own, qkv1, qkv2, w1, w2) = refs[14:37]
    lsem, ssem, rsem = refs[37:40]
    zsems = refs[40:]
    at, wire = Place(nf, ns), Wire(lsem, ssem, rsem)
    own = reduce_start(at, wire, part, acc, other)
    own_qkv = wire.keep(qkv.at[at.me], qkv_in.at[at.me])
    order = line_order(at)
    n_done = nf - rest
    fetch = [wire.keep(done.at[0], held)]
    loads = [wire.keep(todo.at[order[n_done + j]], up_own.at[j]) for j in range(rest)]
    at.greet(True, True, True)

    items = [(wout.at[k], w1.at[k], w2.at[k], wout_out.at[k]) for k in range(wout.shape[0])]
    n_out = len(items)
    items += [tuple(ref.at[j] for ref in (up_own, up1, up2, up_sum)) for j in range(rest)]
    items += [tuple(ref.at[c] for ref in (qkv_own, qkv1, qkv2, qkv_out)) for c in range(qkv_own.shape[0])]
    line = LineSum(at, items, zsems)
    for k in range(n_out):
        line.launch(k)
    for j in range(rest):
        loads[j].wait()
        line.launch(n_out + j)

    main = reduce_in_plane(at, wire, own, part, acc, other, ra, rb, rx, ry)
    next(main)
    qkv_moves = [wire.near(qkv.at[p], qkv_in.at[at.me], p) for p in at.plane_peers()]
    row_moves = [wire.near(done.at[j], rows_out.at[at.me], order[j]) for j in range(1, n_done)]
    fetch[0].wait()
    fetch.append(wire.keep(held, rows_out.at[at.me]))

    def arrive_qkv():
        own_qkv.wait()
        for copy in qkv_moves:
            copy.wait_recv()
        group = nf // qkv_own.shape[0]

        def one(i):
            where = pl.ds(pl.multiple_of(i * 16, 16), 16)
            for c in range(qkv_own.shape[0]):
                both = jnp.zeros((16, 2 * HD), F32)
                for g in range(group):
                    piece = qkv_in[c * group + g, where]
                    qkv_own[c, where, g * HD : (g + 1) * HD] = piece[:, :HD]
                    both = both + piece[:, HD:].astype(F32)
                qkv_own[c, where, group * HD :] = both.astype(BF16)

        each(qkv_own.shape[1] // 16, one)
        for c in range(qkv_own.shape[0]):
            line.launch(n_out + rest + c)

    def others():
        yield from main
        gl[...] = terms[...]
        work_on_sum(body, acc, other, rx, ry, (tokens, hid_grad, gain), (gl.at[pl.ds(0, 1)],), block)
        going = go_home(at, wire, block, bz, tok_out)
        next(going)
        gp[at.me] = gl[...]
        small = [wire.near(gl, gp.at[at.me], p) for p in at.plane_peers()]
        yield
        for copy in small:
            copy.wait_recv()
        total = gp[0]
        for k in range(1, nf):
            total = total + gp[k]
        gt[...] = total
        gz[at.z] = total
        small2 = [wire.send(gt, gz.at[at.z], {"seq": p}) for p in at.line_peers()]
        yield
        next(going)
        yield
        for copy in small2:
            copy.wait_recv()
        total = gz[0]
        for k in range(1, ns):
            total = total + gz[k]
        gain_out[...] = total
        for _ in going:
            pass
        for copy in row_moves:
            copy.wait_recv()

    def finished(j):
        item = n_out + j

        @pl.when(line.outer)
        def _():
            line.copy(2, item).wait_recv()

        @pl.when(line.inner)
        def _():
            line.kept(item).wait()

        row_moves.append(wire.near(up_sum.at[j], rows_out.at[at.me], order[n_done + j]))

    steps = line.steps()
    slow = others()
    for i in range(2 * (n_out + 1)):
        steps.pop(0)()
        if i % 2 == 1:
            next(slow, None)
    arrive_qkv()
    while len(steps) > 2 * qkv_own.shape[0] - 2:
        steps.pop(0)()
        if len(steps) % 2 == 1:
            next(slow, None)
    next(slow, None)
    for j in range(rest):
        finished(j)
    while steps:
        steps.pop(0)()
        if len(steps) % 2 == 1:
            next(slow, None)
    for _ in slow:
        pass
    for k in range(len(items)):
        line.end_one(k, n_out <= k < n_out + rest)
    for copy in fetch[1:]:
        copy.wait()
    wire.flush()


def line_order(at):
    return (at.me, at.mate, at.xn, at.yn, at.xn + at.step, at.yn + at.step, at.diag, at.diag + at.step)


def leave(nf, ns, body, rest, part, tokens, hid_grad, gain, terms, done, todo, qkv, wout):
    rows, _, r, width = part.shape
    spp = nf // ns
    depth = todo.shape[1]
    vmem, anys = pl.BlockSpec(memory_space=pltpu.VMEM), pl.BlockSpec(memory_space=pl.ANY)
    home = jax.ShapeDtypeStruct((nf, r, width), BF16)
    n_send = 10 + (ns - 1) * spp + 2 * (nf - 1) + (ns - 1) + 2 * (nf - 1)
    heads = (KV, depth, (H // KV + 2) * HD)
    piece = todo.shape[1:]
    n_items = wout.shape[0] + rest + KV
    return pl.pallas_call(
        functools.partial(leave_kernel, nf, ns, body, rest),
        name="leave",
        out_shape=[home, jax.ShapeDtypeStruct((8, width), F32)]
        + [jax.ShapeDtypeStruct(s, BF16) for s in (todo.shape, heads, wout.shape)],
        in_specs=[anys, vmem, vmem, vmem, vmem, anys, anys, anys, vmem],
        out_specs=[anys, vmem, anys, anys, anys],
        scratch_shapes=sum_scratch(rows, r, width)
        + [pltpu.VMEM((nf, r, width), BF16)]
        + [pltpu.VMEM((8, width), F32)] * 2
        + [pltpu.VMEM((nf, 8, width), F32), pltpu.VMEM((ns, 8, width), F32)]
        + [pltpu.VMEM(piece, BF16)]
        + [pltpu.VMEM((rest,) + piece, BF16)] * 4
        + [pltpu.VMEM(qkv.shape, BF16)]
        + [pltpu.VMEM(heads, BF16)] * 3
        + [pltpu.VMEM(wout.shape, BF16)] * 2
        + [pltpu.SemaphoreType.DMA((5 + 3 + rest + spp + 4,))]
        + [pltpu.SemaphoreType.DMA((n_send,))] * 2
        + LineSum.semaphores(n_items),
        compiler_params=pltpu.CompilerParams(collective_id=5, has_side_effects=True),
    )(part, tokens, hid_grad, gain, terms, done, todo, qkv, wout)


def whole(a):
    zeros = (0,) * a.ndim
    return pl.BlockSpec(a.shape, lambda i: zeros, pipeline_mode=pl.Buffered(1))


def row_blocks(step, columns):
    return pl.BlockSpec((step, columns), lambda i: (i, 0))


def capped(q, k, last):
    t = jnp.tanh(dot_nt(q, k) * (QUERY_FACTOR / SOFT_CAP))
    e = jnp.exp(SOFT_CAP * t)
    rows = lax.broadcasted_iota(jnp.int32, (last, last), 0)
    columns = lax.broadcasted_iota(jnp.int32, (last, last), 1)
    own = jnp.where(columns <= rows, e[:, e.shape[1] - last :], 0.0)
    e = own if e.shape[1] == last else jnp.concatenate([e[:, : e.shape[1] - last], own], axis=1)
    return t, e, 1.0 / jnp.sum(e, axis=1, keepdims=True)


def attention(a_full, w_qkv, w_out, length):
    tokens, width = a_full.shape
    block = min(256, length)

    def kernel(a, wq, wo, qkv, o, y):
        qkv[...] = dot_f32(a[...], wq[...]).astype(BF16)
        for b in range(length // block):
            rows, keys = pl.ds(b * block, block), pl.ds(0, (b + 1) * block)
            _, e, inv = capped(qkv[rows, :HD], qkv[keys, HD : 2 * HD], block)
            out = dot_f32((e * inv).astype(BF16), qkv[keys, 2 * HD :]).astype(BF16)
            o[rows] = out
            y[rows] = dot_f32(out, wo[...]).astype(BF16)

    return pl.pallas_call(
        kernel,
        name="attention",
        grid=(tokens // length,),
        out_shape=[jax.ShapeDtypeStruct((tokens, c), BF16) for c in (3 * HD, HD, width)],
        in_specs=[row_blocks(length, width), whole(w_qkv), whole(w_out)],
        out_specs=[row_blocks(length, c) for c in (3 * HD, HD, width)],
    )(a_full, w_qkv, w_out)


def attention_back(nf, ns, dy1, qkv, o, a_full, w_qkv, w_out, length, done, todo, count, plan):
    tokens, width = a_full.shape
    block = min(256, length)
    blocks = length // block
    piece = todo.shape[1:]

    def kernel(*refs):
        dy, qk, ov, a, wq, wo, done, todo = refs[:8]
        da, wq_grad, wo_grad, rows_out, summed = refs[8:13]
        acc_q, acc_o, dk, dv, dqkv, held, own, in1, in2, lsem, ssem, rsem = refs[13:25]
        i = pl.program_id(0)
        at = Place(nf, ns)
        order = line_order(at)
        line = LineSum(at, [(own.at[k], in1.at[k], in2.at[k], summed.at[k]) for k in range(count)], refs[25:])
        steps = line.steps()

        def moves():
            return [
                pltpu.make_async_remote_copy(
                    src_ref=done.at[order[j]], dst_ref=rows_out.at[at.me],
                    send_sem=ssem.at[j - 1], recv_sem=rsem.at[j - 1],
                    device_id={"fsdp": order[j]}, device_id_type=MESH,
                )
                for j in range(1, nf)
            ]

        def loads():
            return [pltpu.make_async_copy(todo.at[order[k]], own.at[k], lsem.at[k]) for k in range(count)]

        def held_in():
            return pltpu.make_async_copy(done.at[at.me], held, lsem.at[count])

        def held_out():
            return pltpu.make_async_copy(held, rows_out.at[at.me], lsem.at[count + 1])

        @pl.when(i == 0)
        def _():
            for copy in loads():
                copy.start()
            held_in().start()
            at.greet(False, True, True)
            for k, copy in enumerate(loads()):
                copy.wait()
                line.launch(k)
            for copy in moves():
                copy.start()
            held_in().wait()
            held_out().start()

        out_term = jnp.zeros((HD, width), F32)
        dk[...] = jnp.zeros_like(dk)
        dv[...] = jnp.zeros_like(dv)
        where = 0
        for b in range(blocks):
            rows, keys = pl.ds(b * block, block), pl.ds(0, (b + 1) * block)
            q, k, v = qk[rows, :HD], qk[keys, HD : 2 * HD], qk[keys, 2 * HD :]
            out = ov[rows]
            do = dot_nt(dy[rows], wo[...]).astype(BF16)
            t, e, inv = capped(q, k, block)
            p = e * inv
            dd = jnp.sum(do.astype(F32) * out.astype(F32), axis=1, keepdims=True)
            ds = (p * (dot_nt(do, v) - dd) * (1.0 - t * t) * QUERY_FACTOR).astype(BF16)
            dv[keys] += dot_tn(p.astype(BF16), do)
            dk[keys] += dot_tn(ds, q)
            dqkv[rows, :HD] = dot_f32(ds, k).astype(BF16)
            out_term = out_term + dot_tn(out, dy[rows])
            for turn in range(tokens // length):
                n = plan[turn * blocks + b]
                if n:

                    @pl.when(i == turn)
                    def _():
                        lo = sum(plan[: turn * blocks + b])
                        for step in steps[lo : lo + n]:
                            step()

        dqkv[:, HD : 2 * HD] = dk[...].astype(BF16)
        dqkv[:, 2 * HD :] = dv[...].astype(BF16)
        da[...] = dot_nt(dqkv[...], wq[...]).astype(BF16)
        q_term = dot_tn(a[...], dqkv[...])

        @pl.when(i == 0)
        def _():
            acc_q[...] = q_term
            acc_o[...] = out_term

        @pl.when(i > 0)
        def _():
            acc_q[...] += q_term
            acc_o[...] += out_term

        @pl.when(i == pl.num_programs(0) - 1)
        def _():
            wq_grad[...] = acc_q[...].astype(BF16)
            wo_grad[...] = acc_o[...].astype(BF16)
            for step in steps[sum(plan) :]:
                step()
            line.end()
            held_out().wait()
            for copy in moves():
                copy.wait()

    anys = pl.BlockSpec(memory_space=pl.ANY)
    return pl.pallas_call(
        kernel,
        name="attention_back",
        grid=(tokens // length,),
        out_shape=[
            jax.ShapeDtypeStruct(shape, BF16)
            for shape in ((tokens, width), w_qkv.shape, w_out.shape, done.shape, (count,) + piece)
        ],
        in_specs=[row_blocks(length, c) for c in (width, 3 * HD, HD, width)]
        + [whole(w_qkv), whole(w_out), anys, anys],
        out_specs=[row_blocks(length, width), whole(w_qkv), whole(w_out), anys, anys],
        scratch_shapes=[
            pltpu.VMEM(w_qkv.shape, F32),
            pltpu.VMEM(w_out.shape, F32),
            pltpu.VMEM((length, HD), F32),
            pltpu.VMEM((length, HD), F32),
            pltpu.VMEM((length, 3 * HD), BF16),
            pltpu.VMEM(piece, BF16),
        ]
        + [pltpu.VMEM((count,) + piece, BF16)] * 3
        + [pltpu.SemaphoreType.DMA((count + 2,))]
        + [pltpu.SemaphoreType.DMA((nf - 1,))] * 2
        + LineSum.semaphores(count),
        compiler_params=pltpu.CompilerParams(collective_id=6, has_side_effects=True),
    )(dy1, qkv, o, a_full, w_qkv, w_out, done, todo)


def ffn_forward(n_full, w_gu, w_down, step):
    tokens, width = n_full.shape
    ffp = w_down.shape[0]

    def kernel(n, wg, wd, gu_out, m_out, y):
        gu = dot_f32(n[...], wg[...])
        gu_out[...] = gu.astype(BF16)
        activated, _ = gelu_pair(gu[:, :ffp])
        mixed = (activated * gu[:, ffp:]).astype(BF16)
        m_out[...] = mixed
        y[...] = dot_f32(mixed, wd[...]).astype(BF16)

    return pl.pallas_call(
        kernel,
        name="ffn_forward",
        grid=(tokens // step,),
        out_shape=[jax.ShapeDtypeStruct((tokens, c), BF16) for c in (2 * ffp, ffp, width)],
        in_specs=[row_blocks(step, width), whole(w_gu), whole(w_down)],
        out_specs=[row_blocks(step, c) for c in (2 * ffp, ffp, width)],
    )(n_full, w_gu, w_down)


def ffn_backward(ns, nf, dy2, gu, n_full, w_gu, w_down, step, grad, plan):
    tokens, width = n_full.shape
    ffp = w_down.shape[0]
    turns = tokens // step

    def kernel(*refs):
        dy, gu, n, wg, wd, grad = refs[:6]
        dn, gate_grad, up_grad, summed, acc, in1, in2 = refs[6:13]
        i = pl.program_id(0)
        at = Place(nf, ns)
        count = grad.shape[0]
        line = LineSum(at, [(grad.at[k], in1.at[k], in2.at[k], summed.at[k]) for k in range(count)], refs[13:])
        steps = line.steps()

        @pl.when(i == 0)
        def _():
            at.greet(False, False, True)
            for k in range(count):
                line.launch(k)

        def host(part):
            for turn in range(turns):
                at_plan = turn * 3 + part
                lo, n = sum(plan[:at_plan]), plan[at_plan]
                if n:

                    @pl.when(i == turn)
                    def _():
                        for s in steps[lo : lo + n]:
                            s()

        dm = dot_nt(dy[...], wd[...])
        activated, derivative = gelu_pair(gu[:, :ffp].astype(F32))
        up = gu[:, ffp:].astype(F32)
        dgu = jnp.concatenate(
            [(dm * up * derivative).astype(BF16), (dm * activated).astype(BF16)], axis=1
        )
        host(0)
        dn[...] = dot_nt(dgu, wg[...]).astype(BF16)
        host(1)
        term = dot_tn(n[...], dgu)

        @pl.when(i == 0)
        def _():
            acc[...] = term

        @pl.when(i > 0)
        def _():
            acc[...] += term

        host(2)

        @pl.when(i == turns - 1)
        def _():
            gate_grad[...] = acc[:, :ffp].astype(BF16)
            up_grad[...] = acc[:, ffp:].astype(BF16)
            for s in steps[sum(plan) :]:
                s()
            line.end()

    half = jax.ShapeDtypeStruct((width, ffp), BF16)
    return pl.pallas_call(
        kernel,
        name="ffn_backward",
        grid=(turns,),
        out_shape=[jax.ShapeDtypeStruct((tokens, width), BF16), half, half]
        + [jax.ShapeDtypeStruct(grad.shape, BF16)],
        in_specs=[row_blocks(step, c) for c in (width, 2 * ffp, width)]
        + [whole(w_gu), whole(w_down), whole(grad)],
        out_specs=[row_blocks(step, width), whole(half), whole(half), pl.BlockSpec(memory_space=pl.ANY)],
        scratch_shapes=[pltpu.VMEM(w_gu.shape, F32)]
        + [pltpu.VMEM(grad.shape, BF16)] * 2
        + LineSum.semaphores(grad.shape[0]),
        compiler_params=pltpu.CompilerParams(collective_id=7, has_side_effects=True),
    )(dy2, gu, n_full, w_gu, w_down, grad)


def join_columns(gate, up, heads, nf, ff):
    _, depth, ffp = gate.shape
    n_kv, _, wide = heads.shape
    queries = wide - 2 * HD
    step = 16

    def kernel(x, y, h, out, out_h):
        for g, ref in enumerate((x, y)):
            pieces = [ref[f, :, :ff].astype(F32) for f in range(nf)]
            out[:, g * nf * ff : (g + 1) * nf * ff] = jnp.concatenate(pieces, axis=1)
        for c in range(n_kv):
            piece = h[c].astype(F32)
            out_h[:, c * queries : (c + 1) * queries] = piece[:, :queries]
            for j in range(2):
                lo = n_kv * queries + (j * n_kv + c) * HD
                out_h[:, lo : lo + HD] = piece[:, queries + j * HD : queries + (j + 1) * HD]

    column_spec = pl.BlockSpec((nf, step, ffp), lambda i: (0, i, 0))
    return pl.pallas_call(
        kernel,
        name="join_columns",
        grid=(depth // step,),
        out_shape=[
            jax.ShapeDtypeStruct((depth, 2 * nf * ff), F32),
            jax.ShapeDtypeStruct((depth, n_kv * wide), F32),
        ],
        in_specs=[column_spec] * 2 + [pl.BlockSpec((n_kv, step, wide), lambda i: (0, i, 0))],
        out_specs=[
            pl.BlockSpec((step, 2 * nf * ff), lambda i: (i, 0)),
            pl.BlockSpec((step, n_kv * wide), lambda i: (i, 0)),
        ],
    )(gate, up, heads)


def with_sums(n):
    def mark(f):
        f.n_sums = n
        return f

    return mark


@with_sums(0)
def body_mid(i, branch, ins, outs):
    tokens, gain_attn, gain_ffn = ins
    branch_out, hidden_out = outs
    hidden = tokens[i].astype(F32) + branch * inverse_rms(branch) * gain_attn[...]
    branch_out[i] = branch
    hidden_out[i] = hidden
    return (hidden * inverse_rms(hidden) * gain_ffn[...]).astype(BF16), ()


@with_sums(1)
def body_turn(i, branch, ins, outs):
    hidden, upstream, gain = ins
    scale = inverse_rms(branch)
    outs[0][i] = (hidden[i] + branch * scale * gain[...]).astype(BF16)
    grad, term = norm_back(upstream[i].astype(F32), branch, scale, gain[...])
    return grad.astype(BF16), (term,)


@with_sums(2)
def body_back(i, delta, ins, outs):
    hidden, branch, upstream, gain_attn, gain_ffn = ins
    hid, y1 = hidden[i], branch[i]
    part, term_ffn = norm_back(delta, hid, inverse_rms(hid), gain_ffn[...])
    hid_grad = upstream[i].astype(F32) + part
    outs[0][i] = hid_grad
    grad, term_attn = norm_back(hid_grad, y1, inverse_rms(y1), gain_attn[...])
    return grad.astype(BF16), (term_ffn, term_attn)


@with_sums(1)
def body_last(i, delta, ins, outs):
    tokens, hidden_grad, gain = ins
    values = tokens[i].astype(F32)
    part, term = norm_back(delta, values, inverse_rms(values), gain[...])
    return (hidden_grad[i] + part).astype(BF16), (term,)


def dot_f32(a, b):
    return jnp.dot(a, b, preferred_element_type=F32)


def dot_nt(a, b):
    return lax.dot_general(a, b, (((1,), (1,)), ((), ())), preferred_element_type=F32)


def dot_tn(a, b):
    return lax.dot_general(a, b, (((0,), (0,)), ((), ())), preferred_element_type=F32)


def swap(x, axis):
    return lax.all_to_all(x, axis, split_axis=0, concat_axis=0, tiled=True)


def on_device_plane(
    ns, nf,
    tokens, pre_attn_gain, qkv_weight, out_weight, post_attn_gain, pre_ffn_gain,
    gate_up_weight, down_weight, post_ffn_gain, out_grad,
):
    _, chunk, width = tokens.shape
    length = chunk * ns
    spp = nf // ns
    r = chunk // nf
    rows = spp * ns
    group = H // KV
    ff = down_weight.shape[0]
    ffp = -(-ff // LANES) * LANES
    depth = qkv_weight.shape[0]

    gains = [g.reshape(1, width) for g in (pre_attn_gain, post_attn_gain, pre_ffn_gain, post_ffn_gain)]
    flat = (rows * nf * r, width)
    shape = (rows, nf, r, width)
    tokens_of = min(512, flat[0])

    a_full, x_own, g_own, w_qkv, w_gu = enter(
        nf, ns, tokens.reshape(nf, r, width), out_grad.reshape(nf, r, width), gains[0],
        qkv_weight, gate_up_weight, ffp,
    )
    a_full = a_full.reshape(flat)
    x_own, g_own = x_own.reshape(rows, r, width), g_own.reshape(rows, r, width)
    w_qkv = w_qkv.reshape(nf * depth, 3 * HD)
    w_gu = swap(w_gu, "fsdp").reshape(nf * depth, 2 * ffp)
    w_down = jnp.pad(down_weight, ((0, ffp - ff), (0, 0)))

    qkv, o, y1_terms = attention(a_full, w_qkv, out_weight, length)
    n_full, y1, hidden = middle(
        "mid", 2, nf, ns, body_mid, y1_terms.reshape(shape), [x_own, gains[1], gains[2]], [F32, F32]
    )
    n_full = n_full.reshape(flat)
    gu, mixed, y2_terms = ffn_forward(n_full, w_gu, w_down, tokens_of)
    dy2_full, layer_out, post_ffn_term = middle(
        "turn", 3, nf, ns, body_turn, y2_terms.reshape(shape), [hidden, g_own, gains[3]], [BF16],
        homing=True,
    )
    dy2_full = dy2_full.reshape(flat)
    pieces = next(n for n in (9, 6, 3, 2, 1) if ff % (16 * n) == 0)
    down_wg = dot_tn(mixed, dy2_full)[:ff].astype(BF16).reshape(pieces, ff // pieces, width)
    dn_terms, gate_wg, up_wg, down_wg = ffn_backward(
        ns, nf, dy2_full, gu, n_full, w_gu, w_down, tokens_of, down_wg,
        (0, 0, 1, 0, 2, 2, 0, 2, 2, 0, 2, 0),
    )
    gate_wg, up_wg = gate_wg.reshape(nf, depth, ffp), up_wg.reshape(nf, depth, ffp)
    dy1_full, hidden_grad, pre_ffn_term, post_attn_term, gate_wg = middle(
        "back", 4, nf, ns, body_back, dn_terms.reshape(shape),
        [hidden, y1, g_own, gains[1], gains[2]], [F32],
        grad=gate_wg, plan=(0, 0, 1, 2, 4, 4, 2, 2, 2),
    )
    count = 5
    da_terms, qkv_wg, out_wg, gate_wg, up_sums = attention_back(
        nf, ns, dy1_full.reshape(flat), qkv, o, a_full, w_qkv, out_weight, length,
        gate_wg, up_wg, count, (0, 0, 1, 2, 0, 2, 2, 3),
    )
    terms = jnp.concatenate(
        [jnp.zeros((1, width), F32), post_attn_term, pre_ffn_term, post_ffn_term, jnp.zeros((4, width), F32)]
    )
    tokens_grad, gain_sums, up_wg, qkv_wg, out_wg = leave(
        nf, ns, body_last, nf - count, da_terms.reshape(shape), x_own, hidden_grad, gains[0], terms,
        up_sums, up_wg, qkv_wg.reshape(nf, depth, 3 * HD), out_wg.reshape(2, HD // 2, width),
    )
    gu_wg, qkv_wg = join_columns(gate_wg, up_wg, qkv_wg, nf, ff)
    return (
        layer_out.reshape(1, chunk, width),
        tokens_grad.astype(F32).reshape(1, chunk, width),
        gain_sums[0],
        qkv_wg,
        out_wg.reshape(HD, width).astype(F32),
        gain_sums[1],
        gain_sums[2],
        gu_wg,
        down_wg.reshape(ff, width).astype(F32),
        gain_sums[3],
    )


def gathered_norm_back(upstream, values, inv_scale, gains):
    weighted = upstream * gains
    inner_mean = jnp.mean(weighted * values, axis=-1, keepdims=True)
    gradient = inv_scale * weighted - values * (inv_scale * inv_scale * inv_scale) * inner_mean
    gain_grad = jnp.sum(upstream * values * inv_scale, axis=0)
    return (gradient, gain_grad)


def batched_contraction(pattern, left_side, right_side):
    return jnp.einsum(pattern, left_side, right_side, preferred_element_type=jnp.float32)


def gathered_capped_scores(block_of_queries, key_row_slices, offset):
    amount = block_of_queries.shape[0]
    key_count = key_row_slices.shape[0]
    unscaled_logits = (
        batched_contraction("olv,ilv->loi", block_of_queries, key_row_slices) * QUERY_FACTOR
    )
    tanh_part = jnp.tanh(unscaled_logits / SOFT_CAP)
    allowed = (
        jnp.arange(key_count, dtype=jnp.int32)[None, :]
        <= (offset + jnp.arange(amount, dtype=jnp.int32))[:, None]
    )
    capped = jnp.where(allowed[None], SOFT_CAP * tanh_part, MASKED)
    return (tanh_part, capped)


def gathered_attend(queries, key_row_slices, value_row_slices):
    length = queries.shape[0]
    block_size = min(512, length)
    blocks = length // block_size

    def one_block(block_id):
        offset = block_id * block_size
        block_of_queries = lax.dynamic_slice_in_dim(queries, offset, block_size, 0)
        tanh_part, capped = gathered_capped_scores(block_of_queries, key_row_slices, offset)
        biggest = jnp.max(capped, axis=-1, keepdims=True)
        logsum = biggest + jnp.log(jnp.sum(jnp.exp(capped - biggest), axis=-1, keepdims=True))
        attention_probabilities = jnp.exp(capped - logsum).astype(jnp.bfloat16)
        layer_result = batched_contraction(
            "vxn,nvs->xvs", attention_probabilities, value_row_slices
        ).astype(jnp.bfloat16)
        return (layer_result, logsum[..., 0])

    outputs, logsums = lax.map(one_block, jnp.arange(blocks, dtype=jnp.int32))
    return (outputs.reshape(queries.shape), logsums)


def gathered_attend_back(queries, key_row_slices, value_row_slices, outputs, out_delta, logsums):
    length = queries.shape[0]
    block_size = min(512, length)
    blocks = length // block_size
    row_dots = batched_contraction("qbd,qbd->bq", out_delta, outputs)

    def one_block(carried, inputs):
        key_accumulator, value_accumulator = carried
        block_id, block_logsum = inputs
        offset = block_id * block_size
        block_of_queries = lax.dynamic_slice_in_dim(queries, offset, block_size, 0)
        block_correction = lax.dynamic_slice_in_dim(out_delta, offset, block_size, 0)
        tanh_part, capped = gathered_capped_scores(block_of_queries, key_row_slices, offset)
        attention_probabilities = jnp.exp(capped - block_logsum[..., None])
        probability_gradients = batched_contraction(
            "olv,ilv->loi", block_correction, value_row_slices
        )
        dots_block = lax.dynamic_slice_in_dim(row_dots, offset, block_size, 1)
        logit_gradients = (
            attention_probabilities
            * (probability_gradients - dots_block[..., None])
            * (1.0 - tanh_part * tanh_part)
            * QUERY_FACTOR
        ).astype(jnp.bfloat16)
        rounded_values = attention_probabilities.astype(jnp.bfloat16)
        value_accumulator = value_accumulator + batched_contraction(
            "pfm,fpg->mpg", rounded_values, block_correction
        )
        key_accumulator = key_accumulator + batched_contraction(
            "pfm,fpg->mpg", logit_gradients, block_of_queries
        )
        query_gradient = batched_contraction(
            "vxn,nvs->xvs", logit_gradients, key_row_slices
        ).astype(jnp.bfloat16)
        return ((key_accumulator, value_accumulator), query_gradient)

    zero_acc = jnp.zeros(key_row_slices.shape, jnp.float32)
    (key_accumulator, value_accumulator), query_grads = lax.scan(
        one_block, (zero_acc, zero_acc), (jnp.arange(blocks, dtype=jnp.int32), logsums)
    )
    return (
        query_grads.reshape(queries.shape),
        key_accumulator.astype(jnp.bfloat16),
        value_accumulator.astype(jnp.bfloat16),
    )


def gathered_project(activations, weight_shard):
    return jnp.dot(
        activations,
        lax.all_gather(weight_shard, "fsdp", axis=0, tiled=True),
        preferred_element_type=jnp.float32,
    )


def gathered_project_back(gradient, weight_shard):
    return lax.dot_general(
        gradient,
        lax.all_gather(weight_shard, "fsdp", axis=0, tiled=True),
        (((1,), (1,)), ((), ())),
        preferred_element_type=jnp.float32,
    )


def term_maker(activations, gradient):
    return lax.dot_general(
        activations, gradient, (((0,), (0,)), ((), ())), preferred_element_type=jnp.float32
    )


def weight_term(activations, gradient):
    sliced = lax.psum_scatter(
        term_maker(activations, gradient).astype(jnp.bfloat16),
        "fsdp",
        scatter_dimension=0,
        tiled=True,
    )
    return lax.psum(sliced, "seq").astype(jnp.float32)


def gathered_on_device(
    tokens,
    pre_attn_gain,
    qkv_weight,
    out_weight,
    post_attn_gain,
    pre_ffn_gain,
    gate_up_weight,
    down_weight,
    post_ffn_gain,
    out_grad,
):
    groups, local_len, width = tokens.shape
    row_count = groups * local_len
    head_repeat = H // KV
    ff = gate_up_weight.shape[1] // 2
    residual_in = tokens.reshape(row_count, width).astype(jnp.float32)
    scale_one = inverse_rms(residual_in)
    normed_in = (residual_in * scale_one * pre_attn_gain).astype(jnp.bfloat16)
    projected = gathered_project(normed_in, qkv_weight).astype(jnp.bfloat16)
    queries = projected[:, : H * HD].reshape(groups, local_len, H, HD)
    key_row_slices = jnp.repeat(
        projected[:, H * HD : (H + KV) * HD].reshape(groups, local_len, KV, HD), head_repeat, axis=2
    )
    value_row_slices = jnp.repeat(
        projected[:, (H + KV) * HD :].reshape(groups, local_len, KV, HD), head_repeat, axis=2
    )
    head_queries, head_keys, head_values = (
        lax.all_to_all(queries, "seq", split_axis=2, concat_axis=1, tiled=True),
        lax.all_to_all(key_row_slices, "seq", split_axis=2, concat_axis=1, tiled=True),
        lax.all_to_all(value_row_slices, "seq", split_axis=2, concat_axis=1, tiled=True),
    )
    head_out, logsums = jax.vmap(gathered_attend)(head_queries, head_keys, head_values)
    attn_out = lax.all_to_all(head_out, "seq", split_axis=1, concat_axis=2, tiled=True).reshape(
        row_count, H * HD
    )
    branch_one = gathered_project(attn_out, out_weight)
    scale_two = inverse_rms(branch_one)
    hidden = residual_in + branch_one * scale_two * post_attn_gain
    scale_three = inverse_rms(hidden)
    normed_mid = (hidden * scale_three * pre_ffn_gain).astype(jnp.bfloat16)
    gate_up = gathered_project(normed_mid, gate_up_weight)
    gate_part = gate_up[:, :ff]
    up_part = gate_up[:, ff:]
    activated, derivative = gelu_pair(gate_part)
    mixed = (activated * up_part).astype(jnp.bfloat16)
    branch_two = gathered_project(mixed, down_weight)
    scale_four = inverse_rms(branch_two)
    layer_out = (
        (hidden + branch_two * scale_four * post_ffn_gain)
        .astype(jnp.bfloat16)
        .reshape(groups, local_len, width)
    )
    upstream = out_grad.reshape(row_count, width).astype(jnp.float32)
    branch_two_grad, post_ffn_term = gathered_norm_back(upstream, branch_two, scale_four, post_ffn_gain)
    branch_two_grad = branch_two_grad.astype(jnp.bfloat16)
    down_wgrad = weight_term(mixed, branch_two_grad)
    mixed_grad = gathered_project_back(branch_two_grad, down_weight)
    gate_up_grad = jnp.concatenate(
        [mixed_grad * up_part * derivative, mixed_grad * activated], axis=1
    ).astype(jnp.bfloat16)
    gate_up_wgrad = weight_term(normed_mid, gate_up_grad)
    normed_mid_grad = gathered_project_back(gate_up_grad, gate_up_weight)
    hidden_part, pre_ffn_term = gathered_norm_back(normed_mid_grad, hidden, scale_three, pre_ffn_gain)
    hidden_grad = upstream + hidden_part
    branch_one_grad, post_attn_term = gathered_norm_back(hidden_grad, branch_one, scale_two, post_attn_gain)
    branch_one_grad = branch_one_grad.astype(jnp.bfloat16)
    out_wgrad = weight_term(attn_out, branch_one_grad)
    attn_grad = (
        gathered_project_back(branch_one_grad, out_weight)
        .astype(jnp.bfloat16)
        .reshape(groups, local_len, H, HD)
    )
    head_delta = lax.all_to_all(attn_grad, "seq", split_axis=2, concat_axis=1, tiled=True)
    query_gradient, key_grad, value_grad = jax.vmap(gathered_attend_back)(
        head_queries, head_keys, head_values, head_out, head_delta, logsums
    )
    query_tok, key_tok, value_tok = (
        lax.all_to_all(query_gradient, "seq", split_axis=1, concat_axis=2, tiled=True),
        lax.all_to_all(key_grad, "seq", split_axis=1, concat_axis=2, tiled=True),
        lax.all_to_all(value_grad, "seq", split_axis=1, concat_axis=2, tiled=True),
    )
    key_sum = (
        key_tok.astype(jnp.float32)
        .reshape(groups, local_len, KV, head_repeat, HD)
        .sum(axis=3)
        .astype(jnp.bfloat16)
    )
    value_sum = (
        value_tok.astype(jnp.float32)
        .reshape(groups, local_len, KV, head_repeat, HD)
        .sum(axis=3)
        .astype(jnp.bfloat16)
    )
    qkv_grad = jnp.concatenate(
        [
            query_tok.reshape(row_count, H * HD),
            key_sum.reshape(row_count, KV * HD),
            value_sum.reshape(row_count, KV * HD),
        ],
        axis=1,
    )
    qkv_wgrad = weight_term(normed_in, qkv_grad)
    normed_in_grad = gathered_project_back(qkv_grad, qkv_weight)
    input_part, pre_attn_term = gathered_norm_back(normed_in_grad, residual_in, scale_one, pre_attn_gain)
    tokens_grad = (hidden_grad + input_part).reshape(groups, local_len, width)
    gain_sums = lax.psum(
        (pre_attn_term, post_attn_term, pre_ffn_term, post_ffn_term), ("seq", "fsdp")
    )
    return (
        layer_out,
        tokens_grad,
        gain_sums[0],
        qkv_wgrad,
        out_wgrad,
        gain_sums[1],
        gain_sums[2],
        gate_up_wgrad,
        down_wgrad,
        gain_sums[3],
    )


def solution(mesh):
    ns, nf = mesh.shape["seq"], mesh.shape["fsdp"]
    token_spec, row_spec = P("fsdp", "seq", None), P("fsdp", None)
    in_specs = (
        token_spec, P(), row_spec, row_spec, P(), P(), row_spec, row_spec, P(), token_spec,
    )
    out_specs = (
        token_spec, token_spec, P(), row_spec, row_spec, P(), P(), row_spec, row_spec, P(),
    )

    def on_device(*args):
        if nf == 8 and nf == H and nf % ns == 0 and ns == 4 and args[0].shape[0] == 1:
            return on_device_plane(ns, nf, *args)
        return gathered_on_device(*args)

    return jax.shard_map(
        on_device, mesh=mesh, in_specs=in_specs, out_specs=out_specs, check_vma=False
    )
```
